1024 devices in a mesh: seq: 32 (over z), uly: 8 (over y_lo, x), rep: 4 (over y_hi, core).
Axes of the slice: x: 4, y: 4 (y_hi: 2, y_lo: 2; y = y_hi * 2 + y_lo), z: 32, core: 2. Of those that a mesh axis runs over, the one named last changes fastest.
Arguments:
- queries: bfloat16 [131072, 2048], P(('rep', 'seq', 'uly')), parts along dimension 0, may hold values from -6 to 6
- keys: bfloat16 [131072, 2048], P(('rep', 'seq', 'uly')), parts along dimension 0, may hold values from -6 to 6
- values: bfloat16 [131072, 2048], P(('rep', 'seq', 'uly')), parts along dimension 0, may hold values from -6 to 6
- past_outputs: bfloat16 [2, 131072, 2048], P(None, ('rep', 'seq', 'uly')), parts along dimension 1, may hold values from -6 to 6
- dwa_slot: int32 [2], replicated, may hold values from 0 to 63
- dwa_table: float32 [2, 64], replicated, may hold values from 0.1 to 0.6
Outputs:
- mixed: bfloat16 [131072, 2048], P(('rep', 'seq', 'uly')), parts along dimension 0
The draws below stay inside these ranges and needn't reach their ends.
There are 4 independent parts, one for each index of `rep`. The reference program is written for one: setup_inputs(seed, part) draws one part's arguments, and reference() takes and returns one part's arrays. A program takes and returns all parts, laid end to end along the dimension named above; an argument that names none is the same for every part. Nothing has to cross between parts.
All inputs are finite; a program needn't handle non-finite values.
Results may differ from the reference program's by a relative error of at most 0.0034.
Values may be sent and summed in bfloat16 or wider, within the bound.
A program may use at most 64 MiB of HBM per device.

```python
import jax
import jax.numpy as jnp
from jax import lax

HEADS = 16
HEAD_DIM = 128
PAST = 2
TABLE = 64
TOK_DEV = 128
SPAN = 4
TOKENS = 32768
N_SEQ = 32
N_ULY = 8


def drawn_pair(key):
    base = jax.random.fold_in(key, 7)
    width = HEADS * HEAD_DIM
    query_field = jnp.clip(2.5 * jax.random.normal(jax.random.fold_in(base, 1), (TOKENS, width), jnp.float32), -6.0, 6.0)
    key_field = jnp.clip(jax.random.normal(jax.random.fold_in(base, 2), (TOKENS, width), jnp.float32), -6.0, 6.0)
    return (query_field, key_field)


def draw_queries(key, part):
    return drawn_pair(key)[0].astype(jnp.bfloat16)


def draw_keys(key, part):
    return drawn_pair(key)[1].astype(jnp.bfloat16)


def block_levels(rng, shape, split, low, largest):
    factor_of, own = 1.0, jax.random.fold_in(rng, 6)
    for dim, shards_of in split:
        heights = jnp.exp(jax.random.uniform(jax.random.fold_in(own, dim), (shards_of,), jnp.float32, low / len(split), largest / len(split)))
        factor_of = factor_of * jnp.repeat(heights, shape[dim] // shards_of).reshape([-1 if axis == dim else 1 for axis in range(len(shape))])
    return factor_of


def scatter_about(stream_key, dims, spread, most, cuts=(), held_as=jnp.bfloat16):
    array = jax.random.normal(stream_key, dims, jnp.float32) * spread
    if len(cuts) > 0:
        array = block_levels(stream_key, dims, cuts, -0.22, 0.18) * array
    return jnp.clip(array, min=-most, max=most).astype(held_as)


def setup_inputs(seed: int = 0, part: int = 0) -> dict:
    key_list = jax.random.split(jax.random.key(seed), 7)
    part_keys = jax.random.split(jax.random.fold_in(key_list[6], part), 7)
    return {
        "queries": draw_queries(jax.random.fold_in(jax.random.fold_in(key_list[6], part), 71), part),
        "keys": draw_keys(jax.random.fold_in(jax.random.fold_in(key_list[6], part), 71), part),
        "values": scatter_about(part_keys[2], (TOKENS, HEADS * HEAD_DIM), 1.0, 6.0, ((0, 256),)),
        "past_outputs": scatter_about(part_keys[3], (PAST, TOKENS, HEADS * HEAD_DIM), 1.0, 6.0, ((1, 256),)),
        "dwa_slot": jax.random.randint(key_list[4], (PAST,), 0, TABLE).astype(jnp.int32),
        "dwa_table": jnp.clip(jax.random.uniform(key_list[5], (2, TABLE), jnp.float32, 0.1, 0.6), 0.1, 0.6),
    }


def one_head(items):
    query, key_block, value_block, allowed = items
    scores = jnp.dot(query, key_block.T, preferred_element_type=jnp.float32) * (1.0 / (HEAD_DIM ** 0.5))
    scores = jnp.where(allowed, scores, -jnp.inf)
    top_score = jnp.max(scores, axis=1, keepdims=True)
    prob = jnp.exp(scores - top_score)
    total = jnp.sum(prob, axis=1, keepdims=True)
    weights = prob.astype(jnp.bfloat16)
    summed = jnp.dot(weights, value_block, preferred_element_type=jnp.float32)
    return (summed / total).astype(jnp.bfloat16)


def reference(queries, keys, values, past_outputs, dwa_slot, dwa_table):
    block_rows = N_ULY * TOK_DEV

    def arrange(field):
        return field.reshape(N_SEQ, block_rows, HEADS, HEAD_DIM)

    padding = jnp.zeros((SPAN - 1, block_rows, HEADS, HEAD_DIM), jnp.bfloat16)
    query_all = arrange(queries)
    key_padded = jnp.concatenate([padding, arrange(keys)], axis=0)
    value_padded = jnp.concatenate([padding, arrange(values)], axis=0)

    def one_block(block):
        query_block = lax.dynamic_index_in_dim(query_all, block, 0, keepdims=False)
        key_window = lax.dynamic_slice_in_dim(key_padded, block, SPAN, 0).reshape(SPAN * block_rows, HEADS, HEAD_DIM)
        value_window = lax.dynamic_slice_in_dim(value_padded, block, SPAN, 0).reshape(SPAN * block_rows, HEADS, HEAD_DIM)
        query_pos = block * block_rows + jnp.arange(block_rows, dtype=jnp.int32)
        key_pos = (block - SPAN + 1) * block_rows + jnp.arange(SPAN * block_rows, dtype=jnp.int32)
        allowed = (key_pos[None, :] <= query_pos[:, None]) & (key_pos[None, :] >= 0)
        allowed_heads = jnp.broadcast_to(allowed[None, :, :], (HEADS, block_rows, SPAN * block_rows))
        result = lax.map(one_head, (jnp.transpose(query_block, (1, 0, 2)), jnp.transpose(key_window, (1, 0, 2)), jnp.transpose(value_window, (1, 0, 2)), allowed_heads))
        return jnp.transpose(result, (1, 0, 2))

    attended = lax.map(one_block, jnp.arange(N_SEQ, dtype=jnp.int32))
    attended = attended.reshape(TOKENS, HEADS * HEAD_DIM)
    coef_in = dwa_table[0][dwa_slot]
    coef_out = dwa_table[1][dwa_slot]
    layer_in = jnp.zeros((TOKENS, HEADS * HEAD_DIM), jnp.float32)
    extra = jnp.zeros((TOKENS, HEADS * HEAD_DIM), jnp.float32)
    for index in range(PAST):
        stored = past_outputs[index].astype(jnp.float32)
        layer_in = layer_in + coef_in[index] * stored
        extra = extra + coef_out[index] * stored
    hidden = layer_in + attended.astype(jnp.float32)
    return (hidden + extra).astype(jnp.bfloat16)
```

```python
import functools
import math

import jax
import jax.numpy as jnp
from jax import lax
from jax.experimental import pallas as pl
from jax.experimental.pallas import tpu as pltpu
from jax.sharding import PartitionSpec as P

MESH = pl.DeviceIdType.MESH
HEAD_DIM = 128
SCALE = math.log2(math.e) / math.sqrt(HEAD_DIM)
BF16, F32 = jnp.bfloat16, jnp.float32

PLACES = ((0, 0), (0, 1), (0, 3), (1, 0), (1, 1), (1, 3), (0, 2), (1, 2))
MIRROR = tuple(PLACES.index((dy, (4 - dx) % 4)) for dy, dx in PLACES)

ORDER = (
    ("S0", 0), ("S0", 1), ("S0", 2), ("R1", 0), ("R1", 1), ("C1", 0), ("R1", 2), ("C1", 1), ("C1", 2), ("C0", 0),
    ("R2", 0), ("C2", 0), ("C0", 1), ("R2", 1), ("C2", 1), ("C0", 2), ("R2", 2), ("C2", 2), ("C0", 3), ("C3", 0),
    ("S0", 3), ("C3", 1), ("S0", 4), ("C0", 4), ("C3", 2), ("S0", 5), ("C0", 5), ("M2", 0), ("C0", 6), ("R1", 3),
    ("C1", 3), ("M2", 1), ("C0", 7), ("R1", 4), ("C1", 4), ("M2", 2), ("R1", 5), ("C1", 5), ("M1", 0), ("R2", 3),
    ("C2", 3), ("M1", 1), ("R2", 4), ("C2", 4), ("M1", 2), ("R2", 5), ("C2", 5), ("M0", 0), ("C3", 3), ("M0", 1),
    ("S0", 6), ("C3", 4), ("M0", 2), ("S0", 7), ("C3", 5), ("M2", 3), ("R1", 6), ("C1", 6), ("M2", 4), ("R1", 7),
    ("C1", 7), ("M2", 5), ("R2", 6), ("C2", 6), ("M1", 3), ("R2", 7), ("C2", 7), ("M1", 4), ("M1", 5), ("M0", 3),
    ("C3", 6), ("M0", 4), ("C3", 7), ("M0", 5), ("M2", 6), ("M2", 7), ("M1", 6), ("M1", 7), ("M0", 6), ("M0", 7),
)


def kernel(
    q_hbm, k_hbm, v_hbm, out,
    qb, kb, vb, vt, q1, q2, q3, o_in, l_in, o_out, l_out, acc, top, tot, scores, ready,
    ex_send, ex_recv, q_send, q_recv, o_send, l_send, o_recv, l_recv, f_send, f_recv,
):
    z = lax.axis_index("seq")
    n_z = lax.axis_size("seq")
    me = lax.axis_index("uly")
    y, x = me // 4, lax.rem(me, 4)

    def peer(place):
        dy, dx = PLACES[place]
        return lax.rem(y + dy, 2) * 4 + lax.rem(x + dx, 4)

    below, above = z > 0, z < n_z - 1
    barrier = pltpu.get_barrier_semaphore()
    for p in range(1, 8):
        pl.semaphore_signal(barrier, inc=1, device_id={"uly": peer(p)}, device_id_type=MESH)

    @pl.when(below)
    def _():
        pl.semaphore_signal(barrier, inc=1, device_id={"seq": z - 1}, device_id_type=MESH)

    @pl.when(above)
    def _():
        pl.semaphore_signal(barrier, inc=1, device_id={"seq": z + 1}, device_id_type=MESH)

    gathered = ((q_hbm, qb), (k_hbm, kb), (v_hbm, vb))

    def own_copy(t, h):
        src, dst = gathered[t]
        columns = pl.ds(pl.multiple_of((me * 2 + h) * HEAD_DIM, HEAD_DIM), HEAD_DIM)
        return pltpu.make_async_copy(src.at[:, columns], dst.at[h, pl.ds(0, 128)], ex_recv.at[t, h, 0])

    def exchange(t, h, p):
        src, dst = gathered[t]
        to = peer(MIRROR[p])
        columns = pl.ds(pl.multiple_of((to * 2 + h) * HEAD_DIM, HEAD_DIM), HEAD_DIM)
        return pltpu.make_async_remote_copy(
            src_ref=src.at[:, columns], dst_ref=dst.at[h, pl.ds(p * 128, 128)],
            send_sem=ex_send.at[t], recv_sem=ex_recv.at[t, h, p], device_id={"uly": to}, device_id_type=MESH,
        )

    for h in range(2):
        for t in range(3):
            own_copy(t, h).start()

    @pl.when(z == 0)
    def _():
        o_in[...] = jnp.zeros_like(o_in)
        l_in[...] = jnp.full_like(l_in, -1e30)

    pl.semaphore_wait(barrier, 7 + jnp.where(below, 1, 0) + jnp.where(above, 1, 0))

    for h in range(2):
        for t in range(3):
            for p in range(1, 8):
                exchange(t, h, p).start()

    blocks = (qb, q1, q2, q3)

    def rows_of(chunk):
        return chunk // 4, pl.ds((chunk % 4) * 256, 256)

    def down(level, chunk):
        h, rows = rows_of(chunk)
        return pltpu.make_async_remote_copy(
            src_ref=blocks[level].at[h, rows], dst_ref=blocks[level + 1].at[h, rows],
            send_sem=q_send.at[level], recv_sem=q_recv.at[level, chunk],
            device_id={"seq": jnp.maximum(z - 1, 0)}, device_id_type=MESH,
        )

    def up(level, chunk):
        to = jnp.minimum(z + 1, n_z - 1)
        return [
            pltpu.make_async_remote_copy(
                src_ref=src.at[level, chunk], dst_ref=dst.at[level, chunk],
                send_sem=send.at[level], recv_sem=recv.at[level, chunk], device_id={"seq": to}, device_id_type=MESH,
            )
            for src, dst, send, recv in ((o_out, o_in, o_send, o_recv), (l_out, l_in, l_send, l_recv))
        ]

    def finish(chunk, i):
        h, place = chunk // 4, (chunk % 4) * 2 + i
        columns = pl.ds(pl.multiple_of((me * 2 + h) * HEAD_DIM, HEAD_DIM), HEAD_DIM)
        return pltpu.make_async_remote_copy(
            src_ref=ready.at[h, pl.ds(place * 128, 128)], dst_ref=out.at[:, columns],
            send_sem=f_send, recv_sem=f_recv.at[h, MIRROR[place]], device_id={"uly": peer(place)}, device_id_type=MESH,
        )

    def attend(level, chunk):
        h, rows = rows_of(chunk)
        query = blocks[level][h, rows]
        nt = (((1,), (1,)), ((), ()))
        tops = []
        for b in range(4):
            s = lax.dot_general(kb[h, pl.ds(b * 256, 256)], query, nt, preferred_element_type=F32)
            if level == 0:
                key_row = lax.broadcasted_iota(jnp.int32, (256, 1), 0)
                query_row = lax.broadcasted_iota(jnp.int32, (1, 256), 1)
                key_pos = jnp.where(key_row < 128, peer(2 * b) * 128, peer(2 * b + 1) * 128 - 128) + key_row
                first = 2 * (chunk % 4)
                query_pos = jnp.where(query_row < 128, peer(first) * 128, peer(first + 1) * 128 - 128) + query_row
                s = jnp.where(key_pos <= query_pos, s, -1e30)
            scores[pl.ds(b * 256, 256)] = s
            tops.append(jnp.max(s, axis=0, keepdims=True))
        top_ = jnp.maximum(jnp.maximum(tops[0], tops[1]), jnp.maximum(tops[2], tops[3]))
        total = jnp.zeros((1, 256), F32)
        weighted = jnp.zeros((128, 256), F32)
        for b in range(4):
            prob = jnp.exp2((scores[pl.ds(b * 256, 256)] - top_) * SCALE)
            total += jnp.sum(prob, axis=0, keepdims=True)
            weighted += lax.dot_general(
                vt[h, :, pl.ds(b * 256, 256)], prob.astype(BF16), (((1,), (0,)), ((), ())), preferred_element_type=F32
            )
        return weighted, top_ * SCALE, total

    def merged(level, chunk):
        new = l_in[level, chunk]
        own = top[level, chunk]
        most = jnp.maximum(own, new)
        a, b = jnp.exp2(own - most), jnp.exp2(new - most)
        total = tot[level, chunk] * a + b
        weighted = acc[level, chunk] * a + o_in[level, chunk].astype(F32) * b
        return weighted / total, most + jnp.log2(total)

    waited = set()

    def head_ready(h):
        if h in waited:
            return
        waited.add(h)
        for t in (1, 2):
            own_copy(t, h).wait()
            for p in range(1, 8):
                exchange(t, h, p).wait_recv()
        vt[h] = jnp.transpose(vb[h])

    def own_queries(chunk):
        for i in range(2):
            h, p = chunk // 4, (chunk % 4) * 2 + i
            if ("q", h, p) in waited:
                continue
            waited.add(("q", h, p))
            if p == 0:
                own_copy(0, h).wait()
            else:
                exchange(0, h, p).wait_recv()

    def has(level):
        return z < n_z - level

    for step, chunk in ORDER:
        h, rows = rows_of(chunk)
        level = int(step[1])
        if step == "S0":
            own_queries(chunk)

            @pl.when(below)
            def _(chunk=chunk):
                down(0, chunk).start()
        elif step[0] == "R":

            @pl.when(has(level))
            def _(chunk=chunk, level=level):
                down(level - 1, chunk).wait_recv()

            @pl.when(has(level) & below)
            def _(chunk=chunk, level=level):
                down(level, chunk).start()
        elif step == "C3":
            head_ready(h)

            @pl.when(has(3))
            def _(chunk=chunk):
                down(2, chunk).wait_recv()
                weighted, top_, total = attend(3, chunk)
                o_out[2, chunk] = (weighted / total).astype(BF16)
                l_out[2, chunk] = top_ + jnp.log2(total)
                for copy in up(2, chunk):
                    copy.start()
        elif step[0] == "C":
            head_ready(h)
            if level == 0:
                own_queries(chunk)

            @pl.when(has(level))
            def _(chunk=chunk, level=level):
                weighted, top_, total = attend(level, chunk)
                acc[level, chunk] = weighted
                top[level, chunk] = top_
                tot[level, chunk] = total
        elif step == "M0":

            @pl.when(below)
            def _(chunk=chunk):
                for copy in up(0, chunk):
                    copy.wait_recv()

            mean, _unused = merged(0, chunk)
            ready[h, rows] = jnp.transpose(mean).astype(BF16)
            for i in range(2):
                if (chunk % 4) * 2 + i == 0:
                    columns = pl.ds(pl.multiple_of((me * 2 + h) * HEAD_DIM, HEAD_DIM), HEAD_DIM)
                    out[:, columns] = ready[h, pl.ds(0, 128)]
                else:
                    finish(chunk, i).start()
        else:

            @pl.when(has(level) & below)
            def _(chunk=chunk, level=level):
                for copy in up(level, chunk):
                    copy.wait_recv()

            @pl.when(has(level))
            def _(chunk=chunk, level=level):
                mean, log_total = merged(level, chunk)
                o_out[level - 1, chunk] = mean.astype(BF16)
                l_out[level - 1, chunk] = log_total
                for copy in up(level - 1, chunk):
                    copy.start()

    for h in range(2):
        for place in range(1, 8):
            src = pl.ds(pl.multiple_of((peer(place) * 2 + h) * HEAD_DIM, HEAD_DIM), HEAD_DIM)
            pltpu.make_async_remote_copy(
                src_ref=ready.at[h, pl.ds(0, 128)], dst_ref=out.at[:, src],
                send_sem=f_send, recv_sem=f_recv.at[h, place], device_id={"uly": peer(place)}, device_id_type=MESH,
            ).wait_recv()

    for t, (_src, dst) in enumerate(gathered):
        sent = dst.at[:, pl.ds(0, 896)]
        pltpu.make_async_copy(sent, sent, ex_send.at[t]).wait()
    sent = ready.at[:, pl.ds(0, 896)]
    pltpu.make_async_copy(sent, sent, f_send).wait()
    for level in range(3):

        @pl.when(has(level) & below)
        def _(level=level):
            sent = blocks[level]
            pltpu.make_async_copy(sent, sent, q_send.at[level]).wait()

        @pl.when(has(level + 1))
        def _(level=level):
            for src, sem in ((o_out, o_send), (l_out, l_send)):
                sent = src.at[level]
                pltpu.make_async_copy(sent, sent, sem.at[level]).wait()


def attention(queries, keys, values):
    block = pltpu.VMEM((2, 1024, HEAD_DIM), BF16)
    dma = pltpu.SemaphoreType.DMA
    hbm = pl.BlockSpec(memory_space=pl.ANY)
    return pl.pallas_call(
        kernel,
        out_shape=jax.ShapeDtypeStruct(queries.shape, BF16),
        in_specs=[hbm, hbm, hbm],
        out_specs=pl.BlockSpec(memory_space=pltpu.VMEM),
        scratch_shapes=[
            block, block, block, pltpu.VMEM((2, HEAD_DIM, 1024), BF16), block, block, block,
            pltpu.VMEM((3, 8, HEAD_DIM, 256), BF16), pltpu.VMEM((3, 8, 1, 256), F32),
            pltpu.VMEM((3, 8, HEAD_DIM, 256), BF16), pltpu.VMEM((3, 8, 1, 256), F32),
            pltpu.VMEM((3, 8, HEAD_DIM, 256), F32), pltpu.VMEM((3, 8, 1, 256), F32), pltpu.VMEM((3, 8, 1, 256), F32),
            pltpu.VMEM((1024, 256), F32), block,
            dma((3,)), dma((3, 2, 8)), dma((3,)), dma((3, 8)), dma((3,)), dma((3,)), dma((3, 8)), dma((3, 8)),
            dma(()), dma((2, 8)),
        ],
        compiler_params=pltpu.CompilerParams(collective_id=0, has_side_effects=True),
        name="attention",
    )(queries, keys, values)


def shards(queries, keys, values, past_outputs, dwa_slot, dwa_table):
    attended = attention(queries, keys, values)
    onehot = (dwa_slot[:, None] == jnp.arange(dwa_table.shape[1])[None, :]).astype(F32)
    coefs = jnp.dot(onehot, jnp.transpose(dwa_table), precision=lax.Precision.HIGHEST)
    layer_in = jnp.zeros(queries.shape, F32)
    extra = jnp.zeros(queries.shape, F32)
    for index in range(past_outputs.shape[0]):
        stored = past_outputs[index].astype(F32)
        layer_in = layer_in + coefs[index, 0] * stored
        extra = extra + coefs[index, 1] * stored
    hidden = layer_in + attended.astype(F32)
    return (hidden + extra).astype(BF16)


def solution(mesh):
    tokens = P(("rep", "seq", "uly"), None)
    return jax.shard_map(
        shards,
        mesh=mesh,
        in_specs=(tokens, tokens, tokens, P(None, ("rep", "seq", "uly"), None), P(), P()),
        out_specs=tokens,
        check_vma=False,
    )
```

```python
import functools
import math

import jax
import jax.numpy as jnp
from jax import lax
from jax.experimental import pallas as pl
from jax.experimental.pallas import tpu as pltpu
from jax.sharding import PartitionSpec as P

MESH = pl.DeviceIdType.MESH
HEAD_DIM = 128
SCALE = math.log2(math.e) / math.sqrt(HEAD_DIM)
BF16, F32 = jnp.bfloat16, jnp.float32
NT = (((1,), (1,)), ((), ()))
NN = (((1,), (0,)), ((), ()))

PLACES = ((0, 0), (0, 1), (0, 3), (1, 0), (1, 1), (1, 3), (0, 2), (1, 2))
MIRROR = tuple(PLACES.index((dy, (4 - dx) % 4)) for dy, dx in PLACES)

MODES = ((1, 2), (0, 3))
EXCHANGE = ((0, 0, 0, 4), (1, 0, 0, 8), (2, 0, 0, 8), (0, 0, 4, 8), (1, 1, 0, 8), (2, 1, 0, 8), (0, 1, 0, 8))

STEPS = ("S0", "R1", "R2", "C3", "C2", "C1", "C0", "M2", "M1", "M0", "KV", "KF", "SK", "SV")
ORDER = (
    208, 192, 8, 1, 2, 193, 0, 3, 194, 196, 24, 195, 17, 198, 211, 16, 19, 199, 210, 18, 209, 212, 197, 4,
    160, 5, 6, 215, 64, 7, 214, 96, 213, 40, 20, 65, 21, 99, 22, 81, 80, 23, 176, 49, 9, 114, 115, 10,
    48, 11, 50, 113, 112, 12, 66, 13, 117, 161, 25, 116, 67, 131, 26, 130, 51, 27, 14, 15, 82, 118, 129, 119,
    133, 41, 42, 132, 68, 43, 28, 83, 84, 101, 29, 30, 134, 135, 52, 69, 31, 53, 44, 45, 97, 120, 46, 98,
    47, 121, 85, 122, 151, 150, 123, 54, 55, 138, 100, 148, 87, 70, 86, 124, 71, 125, 146, 126, 127, 139, 141, 145,
    142, 143, 154, 140, 137, 102, 149, 103, 158, 157, 128, 155, 159, 147, 156, 153, 136, 144, 152,
)


def kernel(
    slot, table, q_hbm, k_hbm, v_hbm, past_hbm, out,
    qb, kb, vb, vt, q1, q2, q3, kf, vf, vft, o_in, l_in, o_out, l_out, acc, top, tot, scores, ready, past, base, came,
    ex_send, ex_recv, q_send, q_recv, kv_send, kv_recv, o_send, l_send, o_recv, l_recv, f_send, f_recv, past_sem,
):
    z = lax.axis_index("seq")
    n_z = lax.axis_size("seq")
    me = lax.axis_index("uly")
    y, x = me // 4, lax.rem(me, 4)
    below, above = z > 0, z < n_z - 1
    to_lower = {"seq": jnp.maximum(z - 1, 0)}
    to_upper = {"seq": jnp.minimum(z + 1, n_z - 1)}

    def peer(place):
        dy, dx = PLACES[place]
        return lax.rem(y + dy, 2) * 4 + lax.rem(x + dx, 4)

    def has(level):
        return z < n_z - level

    def columns_of(device, h):
        return pl.ds(pl.multiple_of((device * 2 + h) * HEAD_DIM, HEAD_DIM), HEAD_DIM)

    def place_rows(p):
        return pl.ds(p * 128, 128)

    barrier = pltpu.get_barrier_semaphore()
    for p in range(1, 8):
        pl.semaphore_signal(barrier, inc=1, device_id={"uly": peer(p)}, device_id_type=MESH)

    @pl.when(below)
    def _():
        pl.semaphore_signal(barrier, inc=1, device_id=to_lower, device_id_type=MESH)

    @pl.when(above)
    def _():
        pl.semaphore_signal(barrier, inc=1, device_id=to_upper, device_id_type=MESH)

    gathered = ((q_hbm, qb), (k_hbm, kb), (v_hbm, vb))

    def own_copy(t, h):
        src, dst = gathered[t]
        return pltpu.make_async_copy(src.at[:, columns_of(me, h)], dst.at[h, place_rows(0)], ex_recv.at[t, h, 0])

    def exchange(t, h, p):
        src, dst = gathered[t]
        to = peer(MIRROR[p])
        return pltpu.make_async_remote_copy(
            src_ref=src.at[:, columns_of(to, h)], dst_ref=dst.at[h, place_rows(p)],
            send_sem=ex_send.at[t], recv_sem=ex_recv.at[t, h, p], device_id={"uly": to}, device_id_type=MESH,
        )

    for h in range(2):
        for t in range(3):
            own_copy(t, h).start()
    past_copy = pltpu.make_async_copy(past_hbm, past, past_sem)
    past_copy.start()

    @pl.when(z == 0)
    def _():
        o_in[...] = jnp.zeros_like(o_in)
        l_in[...] = jnp.full_like(l_in, -1e30)
        kf[...] = jnp.zeros_like(kf)
        vf[...] = jnp.zeros_like(vf)

    past_copy.wait()
    coefs = [table[0, slot[i]] + table[1, slot[i]] for i in range(2)]

    def stored_sum(i, carry):
        rows = pl.ds(pl.multiple_of(i * 16, 16), 16)
        base[rows] = past[0, rows].astype(F32) * coefs[0] + past[1, rows].astype(F32) * coefs[1]
        return carry

    lax.fori_loop(0, 8, stored_sum, 0)

    pl.semaphore_wait(barrier, 7 + jnp.where(below, 1, 0) + jnp.where(above, 1, 0))

    for t, h, first, last in EXCHANGE:
        for p in range(max(first, 1), last):
            exchange(t, h, p).start()

    blocks = (qb, q1, q2, q3)

    def split(chunk):
        return chunk // 8, place_rows(chunk % 8)

    def down(level, chunk):
        h, rows = split(chunk)
        return pltpu.make_async_remote_copy(
            src_ref=blocks[level].at[h, rows], dst_ref=blocks[level + 1].at[h, rows],
            send_sem=q_send.at[level, h], recv_sem=q_recv.at[level, chunk], device_id=to_lower, device_id_type=MESH,
        )

    def forward(t, chunk):
        h, rows = split(chunk)
        src, dst = ((kb, kf), (vb, vf))[t]
        return pltpu.make_async_remote_copy(
            src_ref=src.at[h, rows], dst_ref=dst.at[h, rows],
            send_sem=kv_send.at[t, h], recv_sem=kv_recv.at[t, chunk], device_id=to_upper, device_id_type=MESH,
        )

    def up(level, chunk):
        h = chunk // 8
        return [
            pltpu.make_async_remote_copy(
                src_ref=src.at[level, chunk], dst_ref=dst.at[level, chunk],
                send_sem=send.at[level, h], recv_sem=recv.at[level, chunk], device_id=to_upper, device_id_type=MESH,
            )
            for src, dst, send, recv in ((o_out, o_in, o_send, o_recv), (l_out, l_in, l_send, l_recv))
        ]

    def finish(chunk):
        h, rows = split(chunk)
        place = chunk % 8
        return pltpu.make_async_remote_copy(
            src_ref=ready.at[h, rows], dst_ref=came.at[MIRROR[place], h], send_sem=f_send,
            recv_sem=f_recv.at[MIRROR[place], h], device_id={"uly": peer(place)}, device_id_type=MESH,
        )

    done = set()

    def expect(*wanted):
        by_condition = {}
        for condition, key, copies in wanted:
            if key not in done:
                done.add(key)
                by_condition.setdefault(id(condition), (condition, []))[1].extend(copies)
        for condition, copies in by_condition.values():

            def wait(copies=copies):
                for copy in copies:
                    copy()

            if condition is None:
                wait()
            else:
                pl.when(condition)(wait)

    exists = [None, has(1), has(2), has(3)]
    came_up = [below, has(1) & below, has(2) & below]

    def gathered_rows(t, h, p):
        copy = own_copy(t, h).wait if p == 0 else exchange(t, h, p).wait_recv
        return (None, ("gathered", t, h, p), [copy])

    def queries(level, chunk):
        if level == 0:
            return gathered_rows(0, chunk // 8, chunk % 8)
        return (exists[level], ("down", level, chunk), [down(level - 1, chunk).wait_recv])

    def part(level, chunk):
        return (came_up[level], ("up", level, chunk), [copy.wait_recv for copy in up(level, chunk)])

    def first_stage(step, pair, buffer):
        level = int(step[1])
        h, rows = pair // 4, pl.ds((pair % 4) * 256, 256)
        keys = kb
        source = blocks[level]
        if level == 3 and MODES[h][0] == 1:
            keys, source = kf, q2
        query = source[h, rows]
        tops = []
        for b in range(4):
            s = lax.dot_general(keys[h, pl.ds(b * 256, 256)], query, NT, preferred_element_type=F32)
            if level == 0:
                key_row = lax.broadcasted_iota(jnp.int32, (256, 1), 0)
                query_row = lax.broadcasted_iota(jnp.int32, (1, 256), 1)
                key_pos = jnp.where(key_row < 128, peer(2 * b) * 128, peer(2 * b + 1) * 128 - 128) + key_row
                first = 2 * (pair % 4)
                query_pos = jnp.where(query_row < 128, peer(first) * 128, peer(first + 1) * 128 - 128) + query_row
                s = jnp.where(key_pos <= query_pos, s, -1e30)
            scores[buffer, pl.ds(b * 256, 256)] = s
            tops.append(jnp.max(s.reshape(32, 8, 256), axis=0))
        tops = jnp.maximum(jnp.maximum(tops[0], tops[1]), jnp.maximum(tops[2], tops[3]))
        return jnp.max(tops, axis=0, keepdims=True)

    def second_stage(step, pair, buffer, highest):
        level = int(step[1])
        h = pair // 4
        values = vft if level == 3 and MODES[h][0] == 1 else vt
        total = jnp.zeros((8, 256), F32)
        weighted = None
        for b in range(4):
            prob = jnp.exp2((scores[buffer, pl.ds(b * 256, 256)] - highest) * SCALE)
            total += jnp.sum(prob.reshape(32, 8, 256), axis=0)
            term = lax.dot_general(
                values[h, :, pl.ds(b * 256, 256)], prob.astype(BF16), NN, preferred_element_type=F32
            )
            weighted = term if weighted is None else weighted + term
        return weighted, jnp.sum(total, axis=0, keepdims=True)

    pending = []
    turn = [0]

    def advance(step=None, pair=None):
        last = pending.pop() if pending else None
        if step is not None:
            buffer = turn[0] % 2
            turn[0] += 1
            level = int(step[1])
            highest = first_stage(step, pair, buffer)
        if last is not None:
            old_step, old_pair, old_buffer = last
            old = int(old_step[1])
            old_top = top[old, old_pair]
            weighted, total = second_stage(old_step, old_pair, old_buffer, old_top)
            if old == 3 and MODES[old_pair // 4][1] == 3:
                mean = (weighted / total).astype(BF16)
                log_total = old_top * SCALE + jnp.log2(total)
                for i in range(2):
                    o_out[2, 2 * old_pair + i] = mean[:, i * 128 : i * 128 + 128]
                    l_out[2, 2 * old_pair + i] = log_total[:, i * 128 : i * 128 + 128]
            else:
                acc[old, old_pair] = weighted
                tot[old, old_pair] = total
                if old == 3:
                    top[old, old_pair] = jnp.where(below, old_top, -1e30)
        if step is not None:
            top[level, pair] = highest
            pending.append((step, pair, buffer))
        if last is not None and old == 3 and MODES[old_pair // 4][1] == 3:

            @pl.when(has(3))
            def _():
                for i in range(2):
                    for copy in up(2, 2 * old_pair + i):
                        copy.start()

    def settle(*units):
        if pending and pending[0][:2] in units:
            advance()

    def merged(chunk, level):
        pair, lanes = chunk // 2, slice(chunk % 2 * 128, chunk % 2 * 128 + 128)
        own = top[level, pair][:, lanes] * SCALE
        if level == 2 and MODES[chunk // 8][0] == 1:
            new = top[3, pair][:, lanes] * SCALE
            new_total, new_weighted = tot[3, pair][:, lanes], acc[3, pair, :, lanes]
        else:
            new = l_in[level, chunk]
            new_total, new_weighted = 1.0, o_in[level, chunk].astype(F32)
        most = jnp.maximum(own, new)
        a, b = jnp.exp2(own - most), jnp.exp2(new - most)
        total = tot[level, pair][:, lanes] * a + new_total * b
        weighted = acc[level, pair, :, lanes] * a + new_weighted * b
        return weighted / total, most + jnp.log2(total)

    for code in ORDER:
        step, which = STEPS[code // 16], code % 16
        if step in ("S0", "R1", "R2"):
            level = STEPS.index(step)
            expect(queries(level, which))
            pl.when(has(level) & below)(down(level, which).start)
        elif step in ("SK", "SV"):
            t = STEPS.index(step) - STEPS.index("SK")
            expect(gathered_rows(t + 1, which // 8, which % 8))
            pl.when(above)(forward(t, which).start)
        elif step == "KV":
            expect(*(gathered_rows(t, which, p) for t in (1, 2) for p in range(8)))
            vt[which] = jnp.transpose(vb[which])
        elif step == "KF":
            chunks = range(which * 8, which * 8 + 8)
            expect(*((below, ("kf", t, c), [forward(t, c).wait_recv]) for t in (0, 1) for c in chunks))
            vft[which] = jnp.transpose(vf[which])
        elif step[0] == "C":
            level = int(step[1])
            if level == 3 and MODES[which // 4][0] == 1:
                level = 2
            expect(queries(level, 2 * which), queries(level, 2 * which + 1))
            advance(step, which)
        elif step == "M0":
            settle(("C0", which // 2))
            expect(part(0, which))
            mean, _unused = merged(which, 0)
            h, rows = split(which)
            if which % 8 == 0:
                came[0, h] = jnp.transpose(mean).astype(BF16)
            else:
                ready[h, rows] = jnp.transpose(mean).astype(BF16)
                finish(which).start()
        else:
            level = int(step[1])
            if level == 2 and MODES[which // 8][0] == 1:
                settle(("C2", which // 2), ("C3", which // 2))
            else:
                settle((f"C{level}", which // 2))
                expect(part(level, which))
            mean, log_total = merged(which, level)
            o_out[level - 1, which] = mean.astype(BF16)
            l_out[level - 1, which] = log_total

            @pl.when(has(level))
            def _(level=level, which=which):
                for copy in up(level - 1, which):
                    copy.start()

    for code in ORDER:
        step, which = STEPS[code // 16], code % 16
        if step == "M0":
            h, place = which // 8, MIRROR[which % 8]
            if place:
                pltpu.make_async_remote_copy(
                    src_ref=ready.at[h, place_rows(place)], dst_ref=came.at[place, h], send_sem=f_send,
                    recv_sem=f_recv.at[place, h], device_id={"uly": peer(place)}, device_id_type=MESH,
                ).wait_recv()
            lanes = columns_of(peer(place), h)
            out[:, lanes] = (base[:, lanes] + came[place, h].astype(F32)).astype(BF16)

    for t, (_src, dst) in enumerate(gathered):
        sent = dst.at[:, pl.ds(0, 896)]
        pltpu.make_async_copy(sent, sent, ex_send.at[t]).wait()
    sent = ready.at[:, pl.ds(0, 896)]
    pltpu.make_async_copy(sent, sent, f_send).wait()

    def all_left(condition, sent, sem):
        pl.when(condition)(pltpu.make_async_copy(sent, sent, sem).wait)

    for h, (up_hops, down_hops) in enumerate(MODES):
        chunks = pl.ds(h * 8, 8)
        for level in range(down_hops):
            all_left(has(level) & below, blocks[level].at[h], q_send.at[level, h])
            all_left(has(level + 1), o_out.at[level, chunks], o_send.at[level, h])
            all_left(has(level + 1), l_out.at[level, chunks], l_send.at[level, h])
        if up_hops:
            all_left(above, kb.at[h], kv_send.at[0, h])
            all_left(above, vb.at[h], kv_send.at[1, h])


def attention(slot, table, queries, keys, values, past):
    block = pltpu.VMEM((2, 1024, HEAD_DIM), BF16)
    turned = pltpu.VMEM((2, HEAD_DIM, 1024), BF16)
    parts, logs = (3, 16, HEAD_DIM, 128), (3, 16, 1, 128)
    dma = pltpu.SemaphoreType.DMA
    hbm = pl.BlockSpec(memory_space=pl.ANY)
    smem = pl.BlockSpec(memory_space=pltpu.SMEM)
    return pl.pallas_call(
        kernel,
        out_shape=jax.ShapeDtypeStruct(queries.shape, BF16),
        in_specs=[smem, smem, hbm, hbm, hbm, hbm],
        out_specs=pl.BlockSpec(memory_space=pltpu.VMEM),
        scratch_shapes=[
            block, block, block, turned, block, block, block, block, block, turned,
            pltpu.VMEM(parts, BF16), pltpu.VMEM(logs, F32), pltpu.VMEM(parts, BF16), pltpu.VMEM(logs, F32),
            pltpu.VMEM((4, 8, HEAD_DIM, 256), F32), pltpu.VMEM((4, 8, 1, 256), F32), pltpu.VMEM((4, 8, 1, 256), F32),
            pltpu.VMEM((2, 1024, 256), F32), block,
            pltpu.VMEM(past.shape, BF16), pltpu.VMEM(queries.shape, F32), pltpu.VMEM((8, 2, 128, HEAD_DIM), BF16),
            dma((3,)), dma((3, 2, 8)), dma((3, 2)), dma((3, 16)), dma((2, 2)), dma((2, 16)),
            dma((3, 2)), dma((3, 2)), dma((3, 16)), dma((3, 16)), dma(()), dma((8, 2)), dma(()),
        ],
        compiler_params=pltpu.CompilerParams(collective_id=0, has_side_effects=True),
        name="attention",
    )(slot, table, queries, keys, values, past)


def shards(queries, keys, values, past_outputs, dwa_slot, dwa_table):
    return attention(dwa_slot, dwa_table, queries, keys, values, past_outputs)


def solution(mesh):
    tokens = P(("rep", "seq", "uly"), None)
    return jax.shard_map(
        shards,
        mesh=mesh,
        in_specs=(tokens, tokens, tokens, P(None, ("rep", "seq", "uly"), None), P(), P()),
        out_specs=tokens,
        check_vma=False,
    )
```

```python
import functools
import math

import jax
import jax.numpy as jnp
from jax import lax
from jax.experimental import pallas as pl
from jax.experimental.pallas import tpu as pltpu
from jax.sharding import PartitionSpec as P

MESH = pl.DeviceIdType.MESH
HEAD_DIM = 128
SCALE = math.log2(math.e) / math.sqrt(HEAD_DIM)
BF16, F32 = jnp.bfloat16, jnp.float32
NT = (((1,), (1,)), ((), ()))
NN = (((1,), (0,)), ((), ()))

PLACES = ((0, 0), (0, 1), (0, 3), (1, 0), (1, 1), (1, 3), (0, 2), (1, 2))
MIRROR = tuple(PLACES.index((dy, (4 - dx) % 4)) for dy, dx in PLACES)

MODES = ((1, 2), (0, 3))
EXCHANGE = (
    32, 10, 11, 13, 8, 12, 15, 28, 22, 14, 38, 33, 18, 34, 37, 17, 36, 39, 23, 21, 45, 35, 29, 43,
    27, 30, 26, 20, 46, 19, 44, 31, 47, 42, 41, 0, 24, 25, 6, 2, 16, 9, 1, 40, 7, 3, 4, 5,
)

STEPS = ("S0", "R1", "R2", "C3", "C2", "C1", "C0", "M2", "M1", "M0", "KV", "KF", "SK")
ORDER = (
    8, 0, 10, 11, 13, 192, 12, 15, 14, 26, 198, 27, 194, 193, 29, 28, 31, 197, 30, 42, 199, 43, 45, 44,
    195, 47, 46, 24, 196, 161, 53, 9, 2, 54, 69, 70, 3, 55, 7, 85, 5, 4, 71, 122, 25, 123, 18, 124,
    86, 19, 160, 176, 125, 6, 96, 23, 98, 127, 87, 126, 20, 21, 139, 102, 140, 1, 138, 141, 68, 49, 40, 143,
    41, 22, 142, 103, 65, 82, 16, 115, 114, 101, 50, 66, 116, 156, 17, 117, 52, 67, 81, 131, 51, 155, 132, 118,
    100, 157, 48, 119, 99, 130, 121, 133, 64, 113, 120, 84, 83, 135, 80, 134, 159, 148, 149, 97, 137, 129, 158, 112,
    151, 146, 136, 154, 147, 153, 150, 145, 128, 152, 144,
)


M0S = tuple(code % 16 for code in ORDER if STEPS[code // 16] == "M0")
BATCHES = ((0, 8), (8, 10), (10, 12), (12, 13), (13, 14), (14, 15), (15, 16))


def batch_of(chunk):
    at = M0S.index(chunk)
    return next(i for i, (first, last) in enumerate(BATCHES) if first <= at < last)


def kernel(
    slot_hbm, table_hbm, q_hbm, k_hbm, v_hbm, past_hbm, out,
    slot, table, qs, ks, vs, past, base, tally,
    qb, kb, vb, vt, q1, q2, q3, kf, vf, vft, o_in, l_in, o_out, l_out, acc, top, tot, scores, ready, came,
    stage_sem, ex_send, q_ex, kv_ex, q_send, q_recv, kv_send, kv_recv, o_send, o_recv, f_send, f_recv,
):
    z = lax.axis_index("seq")
    n_z = lax.axis_size("seq")
    me = lax.axis_index("uly")
    y, x = me // 4, lax.rem(me, 4)
    below, above = z > 0, z < n_z - 1
    to_lower = {"seq": jnp.maximum(z - 1, 0)}
    to_upper = {"seq": jnp.minimum(z + 1, n_z - 1)}

    def peer(place):
        dy, dx = PLACES[place]
        return lax.rem(y + dy, 2) * 4 + lax.rem(x + dx, 4)

    def has(level):
        return z < n_z - level

    def columns_of(device, h):
        return pl.ds(pl.multiple_of((device * 2 + h) * HEAD_DIM, HEAD_DIM), HEAD_DIM)

    def place_rows(p):
        return pl.ds(p * 128, 128)

    barrier = pltpu.get_barrier_semaphore()
    for p in range(1, 8):
        pl.semaphore_signal(barrier, inc=1, device_id={"uly": peer(p)}, device_id_type=MESH)

    @pl.when(below)
    def _():
        pl.semaphore_signal(barrier, inc=1, device_id=to_lower, device_id_type=MESH)

    @pl.when(above)
    def _():
        pl.semaphore_signal(barrier, inc=1, device_id=to_upper, device_id_type=MESH)

    gathered = ((q_hbm, qs, qb), (k_hbm, ks, kb), (v_hbm, vs, vb))

    def exchange_sem(t, h, p):
        if t == 0:
            return q_ex.at[h, p]
        return kv_ex.at[h, p if MODES[h][0] else 0]

    def own_copy(t, h):
        src, _staged, dst = gathered[t]
        return pltpu.make_async_copy(src.at[:, columns_of(me, h)], dst.at[h, place_rows(0)], exchange_sem(t, h, 0))

    def exchange(t, h, p):
        _src, staged, dst = gathered[t]
        to = peer(MIRROR[p])
        return pltpu.make_async_remote_copy(
            src_ref=staged.at[:, columns_of(to, h)], dst_ref=dst.at[h, place_rows(p)],
            send_sem=ex_send, recv_sem=exchange_sem(t, h, p), device_id={"uly": to}, device_id_type=MESH,
        )

    def stage(t):
        return pltpu.make_async_copy(gathered[t][0], gathered[t][1], stage_sem.at[t])

    stored = [
        pltpu.make_async_copy(src, dst, stage_sem.at[3 + i])
        for i, (src, dst) in enumerate(((past_hbm, past), (slot_hbm, slot), (table_hbm, table)))
    ]
    for t in range(3):
        stage(t).start()
    for h in range(2):
        for t in range(3):
            own_copy(t, h).start()
    for copy in stored:
        copy.start()

    @pl.when(z == 0)
    def _():
        o_in[...] = jnp.zeros_like(o_in)
        l_in[...] = jnp.full_like(l_in, -1e30)
        kf[...] = jnp.zeros_like(kf)
        vf[...] = jnp.zeros_like(vf)

    def stored_sum():
        for copy in stored:
            copy.wait()
        coefs = [table[0, slot[i]] + table[1, slot[i]] for i in range(2)]

        def rows_sum(i, carry):
            rows = pl.ds(pl.multiple_of(i * 16, 16), 16)
            base[rows] = past[0, rows].astype(F32) * coefs[0] + past[1, rows].astype(F32) * coefs[1]
            return carry

        lax.fori_loop(0, 8, rows_sum, 0)

    for t in range(3):
        stage(t).wait()
    pl.semaphore_wait(barrier, 7 + jnp.where(below, 1, 0) + jnp.where(above, 1, 0))

    for code in EXCHANGE:
        if code % 8:
            exchange(code // 16, code // 8 % 2, code % 8).start()

    blocks = (qb, q1, q2, q3)

    def split(chunk):
        return chunk // 8, place_rows(chunk % 8)

    def chunk_base(level):
        return 8 if level == 2 and MODES[0][1] < 3 else 0

    def down(level, chunk):
        h, rows = split(chunk)
        return pltpu.make_async_remote_copy(
            src_ref=blocks[level].at[h, rows], dst_ref=blocks[level + 1].at[h, rows],
            send_sem=q_send.at[level], recv_sem=q_recv.at[level * 16 + chunk - chunk_base(level)],
            device_id=to_lower, device_id_type=MESH,
        )

    def forward(t, chunk):
        h, rows = split(chunk)
        src, dst = ((kb, kf), (vb, vf))[t]
        return pltpu.make_async_remote_copy(
            src_ref=src.at[h, rows], dst_ref=dst.at[h, rows],
            send_sem=kv_send.at[h], recv_sem=kv_recv.at[h], device_id=to_upper, device_id_type=MESH,
        )

    def up(level, chunk):
        at = level * 16 + chunk - chunk_base(level)
        return [
            pltpu.make_async_remote_copy(
                src_ref=src.at[level, chunk], dst_ref=dst.at[level, chunk],
                send_sem=o_send.at[level], recv_sem=o_recv.at[at], device_id=to_upper, device_id_type=MESH,
            )
            for src, dst in ((o_out, o_in), (l_out, l_in))
        ]

    def arrived(semaphore, count):
        pltpu.make_async_copy(tally.at[pl.ds(0, count)], tally.at[pl.ds(0, count)], semaphore).wait()

    def finish(chunk):
        h, rows = split(chunk)
        place = chunk % 8
        return pltpu.make_async_remote_copy(
            src_ref=ready.at[h, rows], dst_ref=came.at[MIRROR[place], h], send_sem=f_send,
            recv_sem=f_recv.at[batch_of(chunk)], device_id={"uly": peer(place)}, device_id_type=MESH,
        )

    done = set()

    def expect(*wanted):
        by_condition = {}
        for condition, key, copies in wanted:
            if key not in done:
                done.add(key)
                by_condition.setdefault(id(condition), (condition, []))[1].extend(copies)
        for condition, copies in by_condition.values():

            def wait(copies=copies):
                for copy in copies:
                    copy()

            if condition is None:
                wait()
            else:
                pl.when(condition)(wait)

    exists = [None, has(1), has(2), has(3)]
    came_up = [below, has(1) & below, has(2) & below]

    def queries(level, chunk):
        h, p = chunk // 8, chunk % 8
        if level == 0:
            return (None, ("queries", h, p), [functools.partial(arrived, exchange_sem(0, h, p), 64)])
        at = (level - 1) * 16 + chunk - chunk_base(level - 1)
        return (exists[level], ("down", level, chunk), [functools.partial(arrived, q_recv.at[at], 64)])

    def keys_values(h, p):
        if MODES[h][0]:
            return (None, ("keys", h, p), [functools.partial(arrived, exchange_sem(1, h, p), 128)])
        return (None, ("keys", h), [functools.partial(arrived, exchange_sem(1, h, p), 1024)])

    def part(level, chunk):
        at = level * 16 + chunk - chunk_base(level)
        return (came_up[level], ("up", level, chunk), [functools.partial(arrived, o_recv.at[at], 65)])

    def first_stage(step, pair, buffer):
        level = int(step[1])
        h, rows = pair // 4, pl.ds((pair % 4) * 256, 256)
        keys = kb
        source = blocks[level]
        if level == 3 and MODES[h][0] == 1:
            keys, source = kf, q2
        query = source[h, rows]
        tops = []
        for b in range(4):
            s = lax.dot_general(keys[h, pl.ds(b * 256, 256)], query, NT, preferred_element_type=F32)
            if level == 0:
                key_row = lax.broadcasted_iota(jnp.int32, (256, 1), 0)
                query_row = lax.broadcasted_iota(jnp.int32, (1, 256), 1)
                key_pos = jnp.where(key_row < 128, peer(2 * b) * 128, peer(2 * b + 1) * 128 - 128) + key_row
                first = 2 * (pair % 4)
                query_pos = jnp.where(query_row < 128, peer(first) * 128, peer(first + 1) * 128 - 128) + query_row
                s = jnp.where(key_pos <= query_pos, s, -1e30)
            scores[buffer, pl.ds(b * 256, 256)] = s
            tops.append(jnp.max(s.reshape(32, 8, 256), axis=0))
        tops = jnp.maximum(jnp.maximum(tops[0], tops[1]), jnp.maximum(tops[2], tops[3]))
        return jnp.max(tops, axis=0, keepdims=True)

    def second_stage(step, pair, buffer, highest):
        level = int(step[1])
        h = pair // 4
        values = vft if level == 3 and MODES[h][0] == 1 else vt
        total = jnp.zeros((8, 256), F32)
        weighted = None
        for b in range(4):
            prob = jnp.exp2((scores[buffer, pl.ds(b * 256, 256)] - highest) * SCALE)
            total += jnp.sum(prob.reshape(32, 8, 256), axis=0)
            term = lax.dot_general(
                values[h, :, pl.ds(b * 256, 256)], prob.astype(BF16), NN, preferred_element_type=F32
            )
            weighted = term if weighted is None else weighted + term
        return weighted, jnp.sum(total, axis=0, keepdims=True)

    pending = []
    turn = [0]

    def advance(step=None, pair=None):
        last = pending.pop() if pending else None
        if step is not None:
            buffer = turn[0] % 2
            turn[0] += 1
            level = int(step[1])
            highest = first_stage(step, pair, buffer)
        if last is not None:
            old_step, old_pair, old_buffer = last
            old = int(old_step[1])
            old_top = top[old, old_pair]
            weighted, total = second_stage(old_step, old_pair, old_buffer, old_top)
            if old == 3 and MODES[old_pair // 4][1] == 3:
                mean = (weighted / total).astype(BF16)
                log_total = old_top * SCALE + jnp.log2(total)
                for i in range(2):
                    o_out[2, 2 * old_pair + i] = mean[:, i * 128 : i * 128 + 128]
                    l_out[2, 2 * old_pair + i] = log_total[:, i * 128 : i * 128 + 128]
            else:
                acc[old, old_pair] = weighted
                tot[old, old_pair] = total
                if old == 3:
                    top[old, old_pair] = jnp.where(below, old_top, -1e30)
        if step is not None:
            top[level, pair] = highest
            pending.append((step, pair, buffer))
        if last is not None and old == 3 and MODES[old_pair // 4][1] == 3:

            @pl.when(has(3))
            def _():
                for i in range(2):
                    for copy in up(2, 2 * old_pair + i):
                        copy.start()

    def settle(*units):
        if pending and pending[0][:2] in units:
            advance()

    def merged(chunk, level):
        pair, lanes = chunk // 2, slice(chunk % 2 * 128, chunk % 2 * 128 + 128)
        own = top[level, pair][:, lanes] * SCALE
        if level == 2 and MODES[chunk // 8][0] == 1:
            new = top[3, pair][:, lanes] * SCALE
            new_total, new_weighted = tot[3, pair][:, lanes], acc[3, pair, :, lanes]
        else:
            new = l_in[level, chunk]
            new_total, new_weighted = 1.0, o_in[level, chunk].astype(F32)
        most = jnp.maximum(own, new)
        a, b = jnp.exp2(own - most), jnp.exp2(new - most)
        total = tot[level, pair][:, lanes] * a + new_total * b
        weighted = acc[level, pair, :, lanes] * a + new_weighted * b
        return weighted / total, most + jnp.log2(total)

    def run(step, which):
        if step in ("S0", "R1", "R2"):
            level = STEPS.index(step)
            expect(queries(level, which))
            pl.when(has(level) & below)(down(level, which).start)
        elif step == "SK":
            expect(keys_values(which // 8, which % 8))

            @pl.when(above)
            def _():
                for t in range(2):
                    forward(t, which).start()
        elif step == "KV":
            expect(*(keys_values(which, p) for p in range(8)))
            vt[which] = jnp.transpose(vb[which])
        elif step == "KF":
            expect((below, ("kf", which), [functools.partial(arrived, kv_recv.at[which], 1024)]))
            vft[which] = jnp.transpose(vf[which])
        elif step[0] == "C":
            level = int(step[1])
            if level == 3 and MODES[which // 4][0] == 1:
                level = 2
            expect(queries(level, 2 * which), queries(level, 2 * which + 1))
            advance(step, which)
        elif step == "M0":
            settle(("C0", which // 2))
            expect(part(0, which))
            mean, _unused = merged(which, 0)
            h, rows = split(which)
            if which % 8 == 0:
                came[0, h] = jnp.transpose(mean).astype(BF16)
            else:
                ready[h, rows] = jnp.transpose(mean).astype(BF16)
                finish(which).start()
        else:
            level = int(step[1])
            if level == 2 and MODES[which // 8][0] == 1:
                settle(("C2", which // 2), ("C3", which // 2))
            else:
                settle((f"C{level}", which // 2))
                expect(part(level, which))
            mean, log_total = merged(which, level)
            o_out[level - 1, which] = mean.astype(BF16)
            l_out[level - 1, which] = log_total

            @pl.when(has(level))
            def _(level=level, which=which):
                for copy in up(level - 1, which):
                    copy.start()

    summed = False
    for code in ORDER:
        step, which = STEPS[code // 16], code % 16
        if not summed and (step not in ("S0", "SK") or which % 8):
            stored_sum()
            summed = True
        run(step, which)

    for batch, (first, last) in enumerate(BATCHES):
        chunks = M0S[first:last]
        remote = sum(1 for chunk in chunks if chunk % 8)
        if remote:
            arrived(f_recv.at[batch], remote * 64)
        for chunk in chunks:
            h, place = chunk // 8, MIRROR[chunk % 8]
            lanes = columns_of(peer(place), h)
            out[:, lanes] = (base[:, lanes] + came[place, h].astype(F32)).astype(BF16)

    sent = scores.at[:, pl.ds(0, 672)]
    pltpu.make_async_copy(sent, sent, ex_send).wait()
    sent = ready.at[:, pl.ds(0, 896)]
    pltpu.make_async_copy(sent, sent, f_send).wait()
    for level in range(3):
        heads = sum(1 for _up_hops, down_hops in MODES if down_hops > level)
        if heads:
            pl.when(has(level) & below)(functools.partial(arrived, q_send.at[level], 512 * heads))
            pl.when(has(level + 1))(functools.partial(arrived, o_send.at[level], 520 * heads))
    for h, (up_hops, _down_hops) in enumerate(MODES):
        if up_hops:
            pl.when(above)(functools.partial(arrived, kv_send.at[h], 1024))


def attention(slot, table, queries, keys, values, past):
    block = pltpu.VMEM((2, 1024, HEAD_DIM), BF16)
    turned = pltpu.VMEM((2, HEAD_DIM, 1024), BF16)
    staged = pltpu.VMEM(queries.shape, BF16)
    parts, logs = (3, 16, HEAD_DIM, 128), (3, 16, 1, 128)
    dma = pltpu.SemaphoreType.DMA
    chunks = 32 + 8 * sum(1 for _up_hops, down_hops in MODES if down_hops == 3)
    return pl.pallas_call(
        kernel,
        out_shape=pltpu.VMEM(queries.shape, BF16),
        in_specs=[pl.BlockSpec(memory_space=pl.ANY)] * 6,
        scratch_shapes=[
            pltpu.SMEM(slot.shape, jnp.int32), pltpu.SMEM(table.shape, F32), staged, staged, staged,
            pltpu.VMEM(past.shape, BF16), pltpu.VMEM(queries.shape, F32), pltpu.VMEM((1040, 1, 128), F32),
            block, block, block, turned, block, block, block, block, block, turned,
            pltpu.VMEM(parts, BF16), pltpu.VMEM(logs, F32), pltpu.VMEM(parts, BF16), pltpu.VMEM(logs, F32),
            pltpu.VMEM((4, 8, HEAD_DIM, 256), F32), pltpu.VMEM((4, 8, 1, 256), F32), pltpu.VMEM((4, 8, 1, 256), F32),
            pltpu.VMEM((2, 1024, 256), F32), block, pltpu.VMEM((8, 2, 128, HEAD_DIM), BF16),
            dma((6,)), dma(()), dma((2, 8)), dma((2, 8)), dma((3,)), dma((chunks,)), dma((2,)), dma((2,)),
            dma((3,)), dma((chunks,)), dma(()), dma((len(BATCHES),)),
        ],
        compiler_params=pltpu.CompilerParams(collective_id=0, has_side_effects=True),
        name="attention",
    )(slot, table, queries, keys, values, past)


def shards(queries, keys, values, past_outputs, dwa_slot, dwa_table):
    return attention(dwa_slot, dwa_table, queries, keys, values, past_outputs)


def solution(mesh):
    tokens = P(("rep", "seq", "uly"), None)
    return jax.shard_map(
        shards,
        mesh=mesh,
        in_specs=(tokens, tokens, tokens, P(None, ("rep", "seq", "uly"), None), P(), P()),
        out_specs=tokens,
        check_vma=False,
    )
```

```python
import functools
import math

import jax
import jax.numpy as jnp
from jax import lax
from jax.experimental import pallas as pl
from jax.experimental.pallas import tpu as pltpu
from jax.sharding import PartitionSpec as P

MESH = pl.DeviceIdType.MESH
HEAD_DIM = 128
SCALE = math.log2(math.e) / math.sqrt(HEAD_DIM)
BF16, F32 = jnp.bfloat16, jnp.float32
NT = (((1,), (1,)), ((), ()))
NN = (((1,), (0,)), ((), ()))

PLACES = ((0, 0), (0, 1), (0, 3), (1, 0), (1, 1), (1, 3), (0, 2), (1, 2))
MIRROR = tuple(PLACES.index((dy, (4 - dx) % 4)) for dy, dx in PLACES)

MODES = ((1, 2), (0, 3))
RAISED = next(h for h, (up_hops, _down_hops) in enumerate(MODES) if up_hops)
EXCHANGE = (
    9, 11, 10, 14, 15, 25, 7, 2, 6, 19, 1, 34, 39, 22, 4, 47, 29, 27, 43, 44, 31, 26, 13, 5,
    12, 20, 18, 35, 28, 42, 3, 45, 30, 46, 41, 37, 38, 21, 36, 33, 23, 17,
)

STEPS = ("S0", "R1", "R2", "C3", "C2", "C1", "C0", "M2", "M1", "M0", "KV", "KF", "SK", "XK", "XI")
ORDER = (
    224, 0, 8, 193, 9, 11, 196, 197, 226, 194, 10, 192, 14, 228, 15, 227, 195, 199, 24, 25, 27, 26, 225, 30,
    31, 40, 41, 43, 42, 198, 46, 47, 161, 87, 13, 215, 210, 213, 229, 12, 5, 4, 84, 7, 52, 6, 53, 55,
    29, 1, 68, 69, 28, 71, 211, 212, 121, 214, 122, 120, 126, 20, 209, 21, 103, 23, 102, 127, 100, 22, 123, 101,
    137, 45, 160, 85, 44, 138, 98, 142, 70, 143, 3, 176, 16, 50, 139, 2, 66, 82, 17, 117, 67, 116, 51, 118,
    158, 54, 19, 119, 86, 153, 96, 18, 133, 99, 83, 132, 64, 48, 81, 134, 80, 125, 113, 124, 65, 49, 135, 115,
    150, 114, 129, 140, 97, 141, 154, 151, 131, 159, 155, 130, 148, 112, 145, 149, 157, 136, 156, 147, 146, 128, 152, 144,
)


M0S = tuple(code % 16 for code in ORDER if STEPS[code // 16] == "M0")
BATCHES = ((0, 8), (8, 11), (11, 13), (13, 14), (14, 15), (15, 16))


def batch_of(chunk):
    at = M0S.index(chunk)
    return next(i for i, (first, last) in enumerate(BATCHES) if first <= at < last)


def kernel(
    slot_hbm, table_hbm, q_hbm, k_hbm, v_hbm, past_hbm, out,
    slot, table, qs, ks, vs, past, base, tally,
    qb, kb, vb, vt, q1, q2, q3, raised, kf, vf, vft, o_in, l_in, o_out, l_out, acc, top, tot, scores, ready, came,
    stage_sem, ex_send, q_ex, kv_ex, q_send, q_recv, kv_send, raised_recv, kf_recv, o_send, f_send, f_recv,
):
    z = lax.axis_index("seq")
    n_z = lax.axis_size("seq")
    me = lax.axis_index("uly")
    y, x = me // 4, lax.rem(me, 4)
    below, above = z > 0, z < n_z - 1
    far_below = z > 1
    to_lower = {"seq": jnp.maximum(z - 1, 0)}
    to_upper = {"seq": jnp.minimum(z + 1, n_z - 1)}

    def peer(place):
        dy, dx = PLACES[place]
        return lax.rem(y + dy, 2) * 4 + lax.rem(x + dx, 4)

    def has(level):
        return z < n_z - level

    def columns_of(device, h):
        return pl.ds(pl.multiple_of((device * 2 + h) * HEAD_DIM, HEAD_DIM), HEAD_DIM)

    def place_rows(p):
        return pl.ds(p * 128, 128)

    barrier = pltpu.get_barrier_semaphore()
    for p in range(1, 8):
        pl.semaphore_signal(barrier, inc=1, device_id={"uly": peer(p)}, device_id_type=MESH)

    @pl.when(below)
    def _():
        pl.semaphore_signal(barrier, inc=1, device_id=to_lower, device_id_type=MESH)

    @pl.when(above & below)
    def _():
        pl.semaphore_signal(barrier, inc=1, device_id=to_upper, device_id_type=MESH)

    gathered = ((q_hbm, qs, qb), (k_hbm, ks, kb), (v_hbm, vs, vb))

    def exchange_sem(t, h, p):
        if t == 0:
            return q_ex.at[h, p]
        return kv_ex.at[h]

    def own_copy(t, h):
        src, _staged, dst = gathered[t]
        return pltpu.make_async_copy(src.at[:, columns_of(me, h)], dst.at[h, place_rows(0)], exchange_sem(t, h, 0))

    def exchange(t, h, p):
        _src, staged, dst = gathered[t]
        to = peer(MIRROR[p])
        return pltpu.make_async_remote_copy(
            src_ref=staged.at[:, columns_of(to, h)], dst_ref=dst.at[h, place_rows(p)],
            send_sem=ex_send.at[0], recv_sem=exchange_sem(t, h, p), device_id={"uly": to}, device_id_type=MESH,
        )

    def stage(t):
        return pltpu.make_async_copy(gathered[t][0], gathered[t][1], stage_sem.at[t])

    stored = [
        pltpu.make_async_copy(src, dst, stage_sem.at[3 + i])
        for i, (src, dst) in enumerate(((past_hbm, past), (slot_hbm, slot), (table_hbm, table)))
    ]
    for t in range(3):
        stage(t).start()
    for h in range(2):
        for t in range(3):
            own_copy(t, h).start()
    for copy in stored:
        copy.start()

    def no_parts():
        o_in[...] = jnp.zeros_like(o_in)
        l_in[...] = jnp.full_like(l_in, -1e30)
        kf[...] = jnp.zeros_like(kf)
        vf[...] = jnp.zeros_like(vf)

    def stored_sum():
        for copy in stored:
            copy.wait()
        coefs = [table[0, slot[i]] + table[1, slot[i]] for i in range(2)]

        def rows_sum(i, carry):
            rows = pl.ds(pl.multiple_of(i * 16, 16), 16)
            base[rows] = past[0, rows].astype(F32) * coefs[0] + past[1, rows].astype(F32) * coefs[1]
            return carry

        lax.fori_loop(0, 8, rows_sum, 0)

    pl.semaphore_wait(barrier, 7 + jnp.where(far_below, 1, 0) + jnp.where(above, 1, 0))

    blocks = (qb, q1, q2, q3)

    def split(chunk):
        return chunk // 8, place_rows(chunk % 8)

    def chunk_base(level):
        return 8 if level == 2 and MODES[0][1] < 3 else 0

    def query_sem(level, chunk):
        if level == 0:
            return q_ex.at[chunk // 8, chunk % 8]
        return q_recv.at[(level - 1) * 16 + chunk - chunk_base(level - 1)]

    def down(level, chunk):
        h, rows = split(chunk)
        return pltpu.make_async_remote_copy(
            src_ref=blocks[level].at[h, rows], dst_ref=blocks[level + 1].at[h, rows],
            send_sem=q_send.at[level], recv_sem=query_sem(level + 1, chunk), device_id=to_lower, device_id_type=MESH,
        )

    def raise_piece(t, p):
        _src, staged, _dst = gathered[t]
        dst = (None, kf, vf)[t].at[place_rows(0)] if p == 0 else raised.at[t - 1, p]
        return pltpu.make_async_remote_copy(
            src_ref=staged.at[:, columns_of(peer(p), RAISED)], dst_ref=dst, send_sem=kv_send,
            recv_sem=kf_recv if p == 0 else raised_recv.at[p], device_id=to_upper, device_id_type=MESH,
        )

    def pass_on(t, p):
        dst = (None, kf, vf)[t]
        return pltpu.make_async_remote_copy(
            src_ref=raised.at[t - 1, p], dst_ref=dst.at[place_rows(MIRROR[p])], send_sem=ex_send.at[1],
            recv_sem=kf_recv, device_id={"uly": peer(p)}, device_id_type=MESH,
        )

    def up(level, chunk):
        return [
            pltpu.make_async_remote_copy(
                src_ref=src.at[level, chunk], dst_ref=dst.at[level, chunk],
                send_sem=o_send.at[level], recv_sem=query_sem(level, chunk), device_id=to_upper, device_id_type=MESH,
            )
            for src, dst in ((o_out, o_in), (l_out, l_in))
        ]

    def arrived(semaphore, count):
        pltpu.make_async_copy(tally.at[pl.ds(0, count)], tally.at[pl.ds(0, count)], semaphore).wait()

    def finish(chunk):
        h, rows = split(chunk)
        place = chunk % 8
        return pltpu.make_async_remote_copy(
            src_ref=ready.at[h, rows], dst_ref=came.at[MIRROR[place], h], send_sem=f_send,
            recv_sem=f_recv.at[batch_of(chunk)], device_id={"uly": peer(place)}, device_id_type=MESH,
        )

    done = set()

    def expect(*wanted):
        by_condition = {}
        for condition, key, copies in wanted:
            if key not in done:
                done.add(key)
                by_condition.setdefault(id(condition), (condition, []))[1].extend(copies)
        for condition, copies in by_condition.values():

            def wait(copies=copies):
                for copy in copies:
                    copy()

            if condition is None:
                wait()
            else:
                pl.when(condition)(wait)

    exists = [None, has(1), has(2), has(3)]
    came_up = [below, has(1) & below, has(2) & below]

    def queries(level, chunk):
        return (exists[level], ("down", level, chunk), [functools.partial(arrived, query_sem(level, chunk), 64)])

    def part(level, chunk):
        return (came_up[level], ("up", level, chunk), [functools.partial(arrived, query_sem(level, chunk), 65)])

    def in_vmem(t):
        return (None, ("in_vmem", t), [lambda: stage(t).wait()])

    def first_stage(step, pair, buffer):
        level = int(step[1])
        h, rows = pair // 4, pl.ds((pair % 4) * 256, 256)
        source = blocks[level]
        if level == 3 and h == RAISED:
            source = q2
        query = source[h, rows]
        tops = []
        for b in range(4):
            of_keys = pl.ds(b * 256, 256)
            keys = kf[of_keys] if level == 3 and h == RAISED else kb[h, of_keys]
            s = lax.dot_general(keys, query, NT, preferred_element_type=F32)
            if level == 0:
                key_row = lax.broadcasted_iota(jnp.int32, (256, 1), 0)
                query_row = lax.broadcasted_iota(jnp.int32, (1, 256), 1)
                key_pos = jnp.where(key_row < 128, peer(2 * b) * 128, peer(2 * b + 1) * 128 - 128) + key_row
                first = 2 * (pair % 4)
                query_pos = jnp.where(query_row < 128, peer(first) * 128, peer(first + 1) * 128 - 128) + query_row
                s = jnp.where(key_pos <= query_pos, s, -1e30)
            scores[buffer, pl.ds(b * 256, 256)] = s
            tops.append(jnp.max(s.reshape(32, 8, 256), axis=0))
        tops = jnp.maximum(jnp.maximum(tops[0], tops[1]), jnp.maximum(tops[2], tops[3]))
        return jnp.max(tops, axis=0, keepdims=True)

    def second_stage(step, pair, buffer, highest):
        level = int(step[1])
        h = pair // 4
        total = jnp.zeros((8, 256), F32)
        weighted = None
        for b in range(4):
            prob = jnp.exp2((scores[buffer, pl.ds(b * 256, 256)] - highest) * SCALE)
            total += jnp.sum(prob.reshape(32, 8, 256), axis=0)
            of_keys = pl.ds(b * 256, 256)
            values = vft[:, of_keys] if level == 3 and h == RAISED else vt[h, :, of_keys]
            term = lax.dot_general(values, prob.astype(BF16), NN, preferred_element_type=F32)
            weighted = term if weighted is None else weighted + term
        return weighted, jnp.sum(total, axis=0, keepdims=True)

    pending = []
    turn = [0]

    def advance(step=None, pair=None):
        last = pending.pop() if pending else None
        if step is not None:
            buffer = turn[0] % 2
            turn[0] += 1
            level = int(step[1])
            highest = first_stage(step, pair, buffer)
        if last is not None:
            old_step, old_pair, old_buffer = last
            old = int(old_step[1])
            old_top = top[old, old_pair]
            weighted, total = second_stage(old_step, old_pair, old_buffer, old_top)
            if old == 3 and MODES[old_pair // 4][1] == 3:
                mean = (weighted / total).astype(BF16)
                log_total = old_top * SCALE + jnp.log2(total)
                for i in range(2):
                    o_out[2, 2 * old_pair + i] = mean[:, i * 128 : i * 128 + 128]
                    l_out[2, 2 * old_pair + i] = log_total[:, i * 128 : i * 128 + 128]
            else:
                acc[old, old_pair] = weighted
                tot[old, old_pair] = total
                if old == 3:
                    top[old, old_pair] = jnp.where(below, old_top, -1e30)
        if step is not None:
            top[level, pair] = highest
            pending.append((step, pair, buffer))
        if last is not None and old == 3 and MODES[old_pair // 4][1] == 3:

            @pl.when(has(3))
            def _():
                for i in range(2):
                    for copy in up(2, 2 * old_pair + i):
                        copy.start()

    def settle(*units):
        if pending and pending[0][:2] in units:
            advance()

    def merged(chunk, level):
        pair, lanes = chunk // 2, slice(chunk % 2 * 128, chunk % 2 * 128 + 128)
        own = top[level, pair][:, lanes] * SCALE
        if level == 2 and MODES[chunk // 8][0] == 1:
            new = top[3, pair][:, lanes] * SCALE
            new_total, new_weighted = tot[3, pair][:, lanes], acc[3, pair, :, lanes]
        else:
            new = l_in[level, chunk]
            new_total, new_weighted = 1.0, o_in[level, chunk].astype(F32)
        most = jnp.maximum(own, new)
        a, b = jnp.exp2(own - most), jnp.exp2(new - most)
        total = tot[level, pair][:, lanes] * a + new_total * b
        weighted = acc[level, pair, :, lanes] * a + new_weighted * b
        return weighted / total, most + jnp.log2(total)

    held = []

    def run(step, which):
        nonlocal held
        if step in ("S0", "R1", "R2"):
            level = STEPS.index(step)
            expect(queries(level, which))
            if held is None:
                pl.when(has(level) & below)(down(level, which).start)
            else:
                pl.when(has(level) & far_below)(down(level, which).start)
                held.append((level, which))
        elif step == "XI":
            for code in EXCHANGE[which * 7 : which * 7 + 7]:
                expect(in_vmem(code // 16))
                exchange(code // 16, code // 8 % 2, code % 8).start()
        elif step == "SK":
            expect(in_vmem(1), in_vmem(2))

            @pl.when(above)
            def _():
                for t in (1, 2):
                    raise_piece(t, which).start()
        elif step == "XK":
            expect((below, ("raised", which), [functools.partial(arrived, raised_recv.at[which], 128)]))

            @pl.when(below)
            def _():
                for t in (1, 2):
                    pass_on(t, which).start()

            if held is not None:
                for level, chunk in held:
                    pl.when(has(level) & (z == 1))(down(level, chunk).start)
                held = None
        elif step == "KV":
            expect((None, ("keys", which), [functools.partial(arrived, kv_ex.at[which], 1024)]))
            vt[which] = jnp.transpose(vb[which])
        elif step == "KF":
            expect((below, ("raised",), [functools.partial(arrived, kf_recv, 1024)]))
            vft[...] = jnp.transpose(vf[...])
        elif step[0] == "C":
            level = int(step[1])
            if level == 3 and MODES[which // 4][0] == 1:
                level = 2
            expect(queries(level, 2 * which), queries(level, 2 * which + 1))
            advance(step, which)
        elif step == "M0":
            settle(("C0", which // 2))
            expect(part(0, which))
            mean, _unused = merged(which, 0)
            h, rows = split(which)
            if which % 8 == 0:
                came[0, h] = jnp.transpose(mean).astype(BF16)
            else:
                ready[h, rows] = jnp.transpose(mean).astype(BF16)
                finish(which).start()
        else:
            level = int(step[1])
            if level == 2 and MODES[which // 8][0] == 1:
                settle(("C2", which // 2), ("C3", which // 2))
            else:
                settle((f"C{level}", which // 2))
                expect(part(level, which))
            mean, log_total = merged(which, level)
            o_out[level - 1, which] = mean.astype(BF16)
            l_out[level - 1, which] = log_total

            @pl.when(has(level))
            def _(level=level, which=which):
                for copy in up(level - 1, which):
                    copy.start()

    summed = False
    for code in ORDER:
        step, which = STEPS[code // 16], code % 16
        if not summed and step not in ("XI", "SK") and which % 8:
            pl.when(z == 0)(no_parts)
            stored_sum()
            summed = True
        run(step, which)

    for batch, (first, last) in enumerate(BATCHES):
        chunks = M0S[first:last]
        remote = sum(1 for chunk in chunks if chunk % 8)
        if remote:
            arrived(f_recv.at[batch], remote * 64)
        for chunk in chunks:
            h, place = chunk // 8, MIRROR[chunk % 8]
            lanes = columns_of(peer(place), h)
            out[:, lanes] = (base[:, lanes] + came[place, h].astype(F32)).astype(BF16)

    sent = scores.at[:, pl.ds(0, 672)]
    pltpu.make_async_copy(sent, sent, ex_send.at[0]).wait()
    sent = ready.at[:, pl.ds(0, 896)]
    pltpu.make_async_copy(sent, sent, f_send).wait()
    pl.when(below)(functools.partial(arrived, ex_send.at[1], 896))
    pl.when(above)(functools.partial(arrived, kv_send, 1024))
    for level in range(3):
        heads = sum(1 for _up_hops, down_hops in MODES if down_hops > level)
        pl.when(has(level) & below)(functools.partial(arrived, q_send.at[level], 512 * heads))
        pl.when(has(level + 1))(functools.partial(arrived, o_send.at[level], 520 * heads))


def attention(slot, table, queries, keys, values, past):
    block = pltpu.VMEM((2, 1024, HEAD_DIM), BF16)
    turned = pltpu.VMEM((2, HEAD_DIM, 1024), BF16)
    staged = pltpu.VMEM(queries.shape, BF16)
    parts, logs = (3, 16, HEAD_DIM, 128), (3, 16, 1, 128)
    dma = pltpu.SemaphoreType.DMA
    chunks = 32 + 8 * sum(1 for _up_hops, down_hops in MODES if down_hops == 3)
    return pl.pallas_call(
        kernel,
        out_shape=pltpu.VMEM(queries.shape, BF16),
        in_specs=[pl.BlockSpec(memory_space=pl.ANY)] * 6,
        scratch_shapes=[
            pltpu.SMEM(slot.shape, jnp.int32), pltpu.SMEM(table.shape, F32), staged, staged, staged,
            pltpu.VMEM(past.shape, BF16), pltpu.VMEM(queries.shape, F32), pltpu.VMEM((1040, 1, 128), F32),
            block, block, block, turned, block, block, block, pltpu.VMEM((2, 8, 128, HEAD_DIM), BF16),
            pltpu.VMEM((1024, HEAD_DIM), BF16), pltpu.VMEM((1024, HEAD_DIM), BF16), pltpu.VMEM((HEAD_DIM, 1024), BF16),
            pltpu.VMEM(parts, BF16), pltpu.VMEM(logs, F32), pltpu.VMEM(parts, BF16), pltpu.VMEM(logs, F32),
            pltpu.VMEM((4, 8, HEAD_DIM, 256), F32), pltpu.VMEM((4, 8, 1, 256), F32), pltpu.VMEM((4, 8, 1, 256), F32),
            pltpu.VMEM((2, 1024, 256), F32), block, pltpu.VMEM((8, 2, 128, HEAD_DIM), BF16),
            dma((6,)), dma((2,)), dma((2, 8)), dma((2,)), dma((3,)), dma((chunks,)), dma(()), dma((8,)), dma(()),
            dma((3,)), dma(()), dma((len(BATCHES),)),
        ],
        compiler_params=pltpu.CompilerParams(collective_id=0, has_side_effects=True),
        name="attention",
    )(slot, table, queries, keys, values, past)


def shards(queries, keys, values, past_outputs, dwa_slot, dwa_table):
    return attention(dwa_slot, dwa_table, queries, keys, values, past_outputs)


def solution(mesh):
    tokens = P(("rep", "seq", "uly"), None)
    return jax.shard_map(
        shards,
        mesh=mesh,
        in_specs=(tokens, tokens, tokens, P(None, ("rep", "seq", "uly"), None), P(), P()),
        out_specs=tokens,
        check_vma=False,
    )
```

```python
import functools
import math

import jax
import jax.numpy as jnp
from jax import lax
from jax.experimental import pallas as pl
from jax.experimental.pallas import tpu as pltpu
from jax.sharding import PartitionSpec as P

MESH = pl.DeviceIdType.MESH
HEAD_DIM = 128
SCALE = math.log2(math.e) / math.sqrt(HEAD_DIM)
BF16, F32 = jnp.bfloat16, jnp.float32
NT = (((1,), (1,)), ((), ()))
NN = (((1,), (0,)), ((), ()))

PLACES = ((0, 0), (0, 1), (0, 3), (1, 0), (1, 1), (1, 3), (0, 2), (1, 2))
MIRROR = tuple(PLACES.index((dy, (4 - dx) % 4)) for dy, dx in PLACES)

MODES = ((1, 2), (0, 3))
RAISED = next(h for h, (up_hops, _down_hops) in enumerate(MODES) if up_hops)
EXCHANGE = (
    9, 11, 10, 14, 15, 25, 7, 2, 6, 19, 1, 34, 39, 22, 4, 47, 29, 27, 43, 44, 31, 26, 13, 5,
    12, 20, 18, 35, 28, 42, 3, 45, 30, 46, 41, 37, 38, 21, 36, 33, 23, 17,
)

STEPS = ("S0", "R1", "R2", "C3", "C2", "C1", "C0", "M2", "M1", "M0", "KV", "KF", "SK", "XK", "XI")
ORDER = (
    224, 0, 8, 193, 9, 11, 196, 197, 226, 194, 10, 192, 14, 228, 15, 227, 195, 199, 24, 25, 27, 26, 225, 30,
    31, 40, 41, 43, 42, 198, 46, 47, 161, 87, 13, 215, 210, 213, 229, 12, 5, 4, 84, 7, 52, 6, 53, 55,
    29, 1, 68, 69, 28, 71, 211, 212, 121, 214, 122, 120, 126, 20, 209, 21, 103, 23, 102, 127, 100, 22, 123, 101,
    137, 45, 160, 85, 44, 138, 98, 142, 70, 143, 3, 176, 16, 50, 139, 2, 66, 82, 17, 117, 67, 116, 51, 118,
    158, 54, 19, 119, 86, 153, 96, 18, 133, 99, 83, 132, 64, 48, 81, 134, 80, 125, 113, 124, 65, 49, 135, 115,
    150, 114, 129, 140, 97, 141, 154, 151, 131, 159, 155, 130, 148, 112, 145, 149, 157, 136, 156, 147, 146, 128, 152, 144,
)


M0S = tuple(code % 16 for code in ORDER if STEPS[code // 16] == "M0")
BATCHES = ((0, 8), (8, 11), (11, 13), (13, 14), (14, 15), (15, 16))


def batch_of(chunk):
    at = M0S.index(chunk)
    return next(i for i, (first, last) in enumerate(BATCHES) if first <= at < last)


def kernel(
    slot_hbm, table_hbm, q_hbm, k_hbm, v_hbm, past_hbm, out,
    slot, table, qs, ks, vs, past, base, tally,
    qb, kb, vb, vt, q1, q2, q3, raised, kf, vf, vft, o_in, l_in, o_out, l_out, acc, top, tot, scores, ready, came,
    stage_sem, ex_send, q_ex, kv_ex, q_send, q_recv, kv_send, raised_recv, kf_recv, o_send, f_send, f_recv,
):
    z = lax.axis_index("seq")
    n_z = lax.axis_size("seq")
    me = lax.axis_index("uly")
    y, x = me // 4, lax.rem(me, 4)
    below, above = z > 0, z < n_z - 1
    far_below = below
    to_lower = {"seq": jnp.maximum(z - 1, 0)}
    to_upper = {"seq": jnp.minimum(z + 1, n_z - 1)}

    def peer(place):
        dy, dx = PLACES[place]
        return lax.rem(y + dy, 2) * 4 + lax.rem(x + dx, 4)

    def has(level):
        return z < n_z - level

    def columns_of(device, h):
        return pl.ds(pl.multiple_of((device * 2 + h) * HEAD_DIM, HEAD_DIM), HEAD_DIM)

    def place_rows(p):
        return pl.ds(p * 128, 128)

    barrier = pltpu.get_barrier_semaphore()
    for p in range(1, 8):
        pl.semaphore_signal(barrier, inc=1, device_id={"uly": peer(p)}, device_id_type=MESH)

    @pl.when(below)
    def _():
        pl.semaphore_signal(barrier, inc=1, device_id=to_lower, device_id_type=MESH)

    @pl.when(above)
    def _():
        pl.semaphore_signal(barrier, inc=1, device_id=to_upper, device_id_type=MESH)

    gathered = ((q_hbm, qs, qb), (k_hbm, ks, kb), (v_hbm, vs, vb))

    def exchange_sem(t, h, p):
        if t == 0:
            return q_ex.at[h, p]
        return kv_ex.at[h]

    def own_copy(t, h):
        src, _staged, dst = gathered[t]
        return pltpu.make_async_copy(src.at[:, columns_of(me, h)], dst.at[h, place_rows(0)], exchange_sem(t, h, 0))

    def exchange(t, h, p):
        _src, staged, dst = gathered[t]
        to = peer(MIRROR[p])
        return pltpu.make_async_remote_copy(
            src_ref=staged.at[:, columns_of(to, h)], dst_ref=dst.at[h, place_rows(p)],
            send_sem=ex_send.at[0], recv_sem=exchange_sem(t, h, p), device_id={"uly": to}, device_id_type=MESH,
        )

    def stage(t):
        return pltpu.make_async_copy(gathered[t][0], gathered[t][1], stage_sem.at[t])

    stored = [
        pltpu.make_async_copy(src, dst, stage_sem.at[3 + i])
        for i, (src, dst) in enumerate(((past_hbm, past), (slot_hbm, slot), (table_hbm, table)))
    ]
    for t in range(3):
        stage(t).start()
    for h in range(2):
        for t in range(3):
            own_copy(t, h).start()
    for copy in stored:
        copy.start()

    def no_parts():
        o_in[...] = jnp.zeros_like(o_in)
        l_in[...] = jnp.full_like(l_in, -1e30)
        kf[...] = jnp.zeros_like(kf)
        vf[...] = jnp.zeros_like(vf)

    def stored_sum():
        for copy in stored:
            copy.wait()
        coefs = [table[0, slot[i]] + table[1, slot[i]] for i in range(2)]

        def rows_sum(i, carry):
            rows = pl.ds(pl.multiple_of(i * 16, 16), 16)
            base[rows] = past[0, rows].astype(F32) * coefs[0] + past[1, rows].astype(F32) * coefs[1]
            return carry

        lax.fori_loop(0, 8, rows_sum, 0)

    pl.semaphore_wait(barrier, 7 + jnp.where(far_below, 1, 0) + jnp.where(above, 1, 0))

    blocks = (qb, q1, q2, q3)

    def split(chunk):
        return chunk // 8, place_rows(chunk % 8)

    def chunk_base(level):
        return 8 if level == 2 and MODES[0][1] < 3 else 0

    def query_sem(level, chunk):
        if level == 0:
            return q_ex.at[chunk // 8, chunk % 8]
        return q_recv.at[(level - 1) * 16 + chunk - chunk_base(level - 1)]

    def down(level, chunk):
        h, rows = split(chunk)
        return pltpu.make_async_remote_copy(
            src_ref=blocks[level].at[h, rows], dst_ref=blocks[level + 1].at[h, rows],
            send_sem=q_send.at[level], recv_sem=query_sem(level + 1, chunk), device_id=to_lower, device_id_type=MESH,
        )

    def raise_piece(t, p):
        _src, staged, _dst = gathered[t]
        dst = (None, kf, vf)[t].at[place_rows(0)] if p == 0 else raised.at[t - 1, p]
        return pltpu.make_async_remote_copy(
            src_ref=staged.at[:, columns_of(peer(p), RAISED)], dst_ref=dst, send_sem=kv_send,
            recv_sem=kf_recv if p == 0 else raised_recv.at[p], device_id=to_upper, device_id_type=MESH,
        )

    def pass_on(t, p):
        dst = (None, kf, vf)[t]
        return pltpu.make_async_remote_copy(
            src_ref=raised.at[t - 1, p], dst_ref=dst.at[place_rows(MIRROR[p])], send_sem=ex_send.at[1],
            recv_sem=kf_recv, device_id={"uly": peer(p)}, device_id_type=MESH,
        )

    def up(level, chunk):
        return [
            pltpu.make_async_remote_copy(
                src_ref=src.at[level, chunk], dst_ref=dst.at[level, chunk],
                send_sem=o_send.at[level], recv_sem=query_sem(level, chunk), device_id=to_upper, device_id_type=MESH,
            )
            for src, dst in ((o_out, o_in), (l_out, l_in))
        ]

    def arrived(semaphore, count):
        pltpu.make_async_copy(tally.at[pl.ds(0, count)], tally.at[pl.ds(0, count)], semaphore).wait()

    def finish(chunk):
        h, rows = split(chunk)
        place = chunk % 8
        return pltpu.make_async_remote_copy(
            src_ref=ready.at[h, rows], dst_ref=came.at[MIRROR[place], h], send_sem=f_send,
            recv_sem=f_recv.at[batch_of(chunk)], device_id={"uly": peer(place)}, device_id_type=MESH,
        )

    done = set()

    def expect(*wanted):
        by_condition = {}
        for condition, key, copies in wanted:
            if key not in done:
                done.add(key)
                by_condition.setdefault(id(condition), (condition, []))[1].extend(copies)
        for condition, copies in by_condition.values():

            def wait(copies=copies):
                for copy in copies:
                    copy()

            if condition is None:
                wait()
            else:
                pl.when(condition)(wait)

    exists = [None, has(1), has(2), has(3)]
    came_up = [below, has(1) & below, has(2) & below]

    def queries(level, chunk):
        return (exists[level], ("down", level, chunk), [functools.partial(arrived, query_sem(level, chunk), 64)])

    def part(level, chunk):
        return (came_up[level], ("up", level, chunk), [functools.partial(arrived, query_sem(level, chunk), 65)])

    def in_vmem(t):
        return (None, ("in_vmem", t), [lambda: stage(t).wait()])

    def first_stage(step, pair, buffer):
        level = int(step[1])
        h, rows = pair // 4, pl.ds((pair % 4) * 256, 256)
        source = blocks[level]
        if level == 3 and h == RAISED:
            source = q2
        query = source[h, rows]
        tops = []
        for b in range(4):
            of_keys = pl.ds(b * 256, 256)
            keys = kf[of_keys] if level == 3 and h == RAISED else kb[h, of_keys]
            s = lax.dot_general(keys, query, NT, preferred_element_type=F32)
            if level == 0:
                key_row = lax.broadcasted_iota(jnp.int32, (256, 1), 0)
                query_row = lax.broadcasted_iota(jnp.int32, (1, 256), 1)
                key_pos = jnp.where(key_row < 128, peer(2 * b) * 128, peer(2 * b + 1) * 128 - 128) + key_row
                first = 2 * (pair % 4)
                query_pos = jnp.where(query_row < 128, peer(first) * 128, peer(first + 1) * 128 - 128) + query_row
                s = jnp.where(key_pos <= query_pos, s, -1e30)
            scores[buffer, pl.ds(b * 256, 256)] = s
            tops.append(jnp.max(s.reshape(32, 8, 256), axis=0))
        tops = jnp.maximum(jnp.maximum(tops[0], tops[1]), jnp.maximum(tops[2], tops[3]))
        return jnp.max(tops, axis=0, keepdims=True)

    def second_stage(step, pair, buffer, highest):
        level = int(step[1])
        h = pair // 4
        total = jnp.zeros((8, 256), F32)
        weighted = None
        for b in range(4):
            prob = jnp.exp2((scores[buffer, pl.ds(b * 256, 256)] - highest) * SCALE)
            total += jnp.sum(prob.reshape(32, 8, 256), axis=0)
            of_keys = pl.ds(b * 256, 256)
            values = vft[:, of_keys] if level == 3 and h == RAISED else vt[h, :, of_keys]
            term = lax.dot_general(values, prob.astype(BF16), NN, preferred_element_type=F32)
            weighted = term if weighted is None else weighted + term
        return weighted, jnp.sum(total, axis=0, keepdims=True)

    pending = []
    turn = [0]

    def advance(step=None, pair=None):
        last = pending.pop() if pending else None
        if step is not None:
            buffer = turn[0] % 2
            turn[0] += 1
            level = int(step[1])
            highest = first_stage(step, pair, buffer)
        if last is not None:
            old_step, old_pair, old_buffer = last
            old = int(old_step[1])
            old_top = top[old, old_pair]
            weighted, total = second_stage(old_step, old_pair, old_buffer, old_top)
            if old == 3 and MODES[old_pair // 4][1] == 3:
                mean = (weighted / total).astype(BF16)
                log_total = old_top * SCALE + jnp.log2(total)
                for i in range(2):
                    o_out[2, 2 * old_pair + i] = mean[:, i * 128 : i * 128 + 128]
                    l_out[2, 2 * old_pair + i] = log_total[:, i * 128 : i * 128 + 128]
            else:
                acc[old, old_pair] = weighted
                tot[old, old_pair] = total
                if old == 3:
                    top[old, old_pair] = jnp.where(below, old_top, -1e30)
        if step is not None:
            top[level, pair] = highest
            pending.append((step, pair, buffer))
        if last is not None and old == 3 and MODES[old_pair // 4][1] == 3:

            @pl.when(has(3))
            def _():
                for i in range(2):
                    for copy in up(2, 2 * old_pair + i):
                        copy.start()

    def settle(*units):
        if pending and pending[0][:2] in units:
            advance()

    def merged(chunk, level):
        pair, lanes = chunk // 2, slice(chunk % 2 * 128, chunk % 2 * 128 + 128)
        own = top[level, pair][:, lanes] * SCALE
        if level == 2 and MODES[chunk // 8][0] == 1:
            new = top[3, pair][:, lanes] * SCALE
            new_total, new_weighted = tot[3, pair][:, lanes], acc[3, pair, :, lanes]
        else:
            new = l_in[level, chunk]
            new_total, new_weighted = 1.0, o_in[level, chunk].astype(F32)
        most = jnp.maximum(own, new)
        a, b = jnp.exp2(own - most), jnp.exp2(new - most)
        total = tot[level, pair][:, lanes] * a + new_total * b
        weighted = acc[level, pair, :, lanes] * a + new_weighted * b
        return weighted / total, most + jnp.log2(total)

    held = None

    def run(step, which):
        nonlocal held
        if step in ("S0", "R1", "R2"):
            level = STEPS.index(step)
            expect(queries(level, which))
            if held is None:
                pl.when(has(level) & below)(down(level, which).start)
            else:
                pl.when(has(level) & far_below)(down(level, which).start)
                held.append((level, which))
        elif step == "XI":
            for code in EXCHANGE[which * 7 : which * 7 + 7]:
                expect(in_vmem(code // 16))
                exchange(code // 16, code // 8 % 2, code % 8).start()
        elif step == "SK":
            expect(in_vmem(1), in_vmem(2))

            @pl.when(above)
            def _():
                for t in (1, 2):
                    raise_piece(t, which).start()
        elif step == "XK":
            expect((below, ("raised", which), [functools.partial(arrived, raised_recv.at[which], 128)]))

            @pl.when(below)
            def _():
                for t in (1, 2):
                    pass_on(t, which).start()

            if held is not None:
                for level, chunk in held:
                    pl.when(has(level) & (z == 1))(down(level, chunk).start)
                held = None
        elif step == "KV":
            expect((None, ("keys", which), [functools.partial(arrived, kv_ex.at[which], 1024)]))
            vt[which] = jnp.transpose(vb[which])
        elif step == "KF":
            expect((below, ("raised",), [functools.partial(arrived, kf_recv, 1024)]))
            vft[...] = jnp.transpose(vf[...])
        elif step[0] == "C":
            level = int(step[1])
            if level == 3 and MODES[which // 4][0] == 1:
                level = 2
            expect(queries(level, 2 * which), queries(level, 2 * which + 1))
            advance(step, which)
        elif step == "M0":
            settle(("C0", which // 2))
            expect(part(0, which))
            mean, _unused = merged(which, 0)
            h, rows = split(which)
            if which % 8 == 0:
                came[0, h] = jnp.transpose(mean).astype(BF16)
            else:
                ready[h, rows] = jnp.transpose(mean).astype(BF16)
                finish(which).start()
        else:
            level = int(step[1])
            if level == 2 and MODES[which // 8][0] == 1:
                settle(("C2", which // 2), ("C3", which // 2))
            else:
                settle((f"C{level}", which // 2))
                expect(part(level, which))
            mean, log_total = merged(which, level)
            o_out[level - 1, which] = mean.astype(BF16)
            l_out[level - 1, which] = log_total

            @pl.when(has(level))
            def _(level=level, which=which):
                for copy in up(level - 1, which):
                    copy.start()

    summed = False
    for code in ORDER:
        step, which = STEPS[code // 16], code % 16
        if not summed and step not in ("XI", "SK") and which % 8:
            pl.when(z == 0)(no_parts)
            stored_sum()
            summed = True
        run(step, which)

    for batch, (first, last) in enumerate(BATCHES):
        chunks = M0S[first:last]
        remote = sum(1 for chunk in chunks if chunk % 8)
        if remote:
            arrived(f_recv.at[batch], remote * 64)
        for chunk in chunks:
            h, place = chunk // 8, MIRROR[chunk % 8]
            lanes = columns_of(peer(place), h)
            out[:, lanes] = (base[:, lanes] + came[place, h].astype(F32)).astype(BF16)

    sent = scores.at[:, pl.ds(0, 672)]
    pltpu.make_async_copy(sent, sent, ex_send.at[0]).wait()
    sent = ready.at[:, pl.ds(0, 896)]
    pltpu.make_async_copy(sent, sent, f_send).wait()
    pl.when(below)(functools.partial(arrived, ex_send.at[1], 896))
    pl.when(above)(functools.partial(arrived, kv_send, 1024))
    for level in range(3):
        heads = sum(1 for _up_hops, down_hops in MODES if down_hops > level)
        pl.when(has(level) & below)(functools.partial(arrived, q_send.at[level], 512 * heads))
        pl.when(has(level + 1))(functools.partial(arrived, o_send.at[level], 520 * heads))


def attention(slot, table, queries, keys, values, past):
    block = pltpu.VMEM((2, 1024, HEAD_DIM), BF16)
    turned = pltpu.VMEM((2, HEAD_DIM, 1024), BF16)
    staged = pltpu.VMEM(queries.shape, BF16)
    parts, logs = (3, 16, HEAD_DIM, 128), (3, 16, 1, 128)
    dma = pltpu.SemaphoreType.DMA
    chunks = 32 + 8 * sum(1 for _up_hops, down_hops in MODES if down_hops == 3)
    return pl.pallas_call(
        kernel,
        out_shape=pltpu.VMEM(queries.shape, BF16),
        in_specs=[pl.BlockSpec(memory_space=pl.ANY)] * 6,
        scratch_shapes=[
            pltpu.SMEM(slot.shape, jnp.int32), pltpu.SMEM(table.shape, F32), staged, staged, staged,
            pltpu.VMEM(past.shape, BF16), pltpu.VMEM(queries.shape, F32), pltpu.VMEM((1040, 1, 128), F32),
            block, block, block, turned, block, block, block, pltpu.VMEM((2, 8, 128, HEAD_DIM), BF16),
            pltpu.VMEM((1024, HEAD_DIM), BF16), pltpu.VMEM((1024, HEAD_DIM), BF16), pltpu.VMEM((HEAD_DIM, 1024), BF16),
            pltpu.VMEM(parts, BF16), pltpu.VMEM(logs, F32), pltpu.VMEM(parts, BF16), pltpu.VMEM(logs, F32),
            pltpu.VMEM((4, 8, HEAD_DIM, 256), F32), pltpu.VMEM((4, 8, 1, 256), F32), pltpu.VMEM((4, 8, 1, 256), F32),
            pltpu.VMEM((2, 1024, 256), F32), block, pltpu.VMEM((8, 2, 128, HEAD_DIM), BF16),
            dma((6,)), dma((2,)), dma((2, 8)), dma((2,)), dma((3,)), dma((chunks,)), dma(()), dma((8,)), dma(()),
            dma((3,)), dma(()), dma((len(BATCHES),)),
        ],
        compiler_params=pltpu.CompilerParams(collective_id=0, has_side_effects=True),
        name="attention",
    )(slot, table, queries, keys, values, past)


def shards(queries, keys, values, past_outputs, dwa_slot, dwa_table):
    return attention(dwa_slot, dwa_table, queries, keys, values, past_outputs)


def solution(mesh):
    tokens = P(("rep", "seq", "uly"), None)
    return jax.shard_map(
        shards,
        mesh=mesh,
        in_specs=(tokens, tokens, tokens, P(None, ("rep", "seq", "uly"), None), P(), P()),
        out_specs=tokens,
        check_vma=False,
    )
```

```python
import functools
import math

import jax
import jax.numpy as jnp
from jax import lax
from jax.experimental import pallas as pl
from jax.experimental.pallas import tpu as pltpu
from jax.sharding import PartitionSpec as P

MESH = pl.DeviceIdType.MESH
HEAD_DIM = 128
SCALE = math.log2(math.e) / math.sqrt(HEAD_DIM)
BF16, F32 = jnp.bfloat16, jnp.float32
NT = (((1,), (1,)), ((), ()))
NN = (((1,), (0,)), ((), ()))

PLACES = ((0, 0), (0, 1), (0, 3), (1, 0), (1, 1), (1, 3), (0, 2), (1, 2))
MIRROR = tuple(PLACES.index((dy, (4 - dx) % 4)) for dy, dx in PLACES)

MODES = ((1, 2), (0, 3))
RAISED = next(h for h, (up_hops, _down_hops) in enumerate(MODES) if up_hops)
EXCHANGE = (
    25, 26, 27, 28, 29, 30, 31, 41, 42, 43, 44, 45, 46, 47, 9, 10, 11, 12, 13, 14, 15, 17, 18, 19,
    20, 21, 22, 23, 33, 34, 35, 36, 37, 38, 39, 1, 2, 3, 4, 5, 6, 7,
)

STEPS = ("S0", "R1", "R2", "C3", "C2", "C1", "C0", "M2", "M1", "M0", "KV", "KF", "SK", "XK", "XI", "FL")
ORDER = (
    15, 196, 199, 195, 11, 197, 198, 192, 194, 10, 14, 12, 13, 8, 9, 224, 225, 226, 27, 26, 31, 30, 212, 28,
    193, 29, 43, 214, 213, 42, 47, 46, 215, 161, 44, 69, 45, 24, 71, 1, 211, 25, 7, 5, 6, 0, 85, 4,
    227, 53, 240, 55, 240, 54, 240, 122, 228, 3, 86, 210, 70, 123, 240, 126, 209, 40, 103, 68, 41, 100, 127, 101,
    87, 23, 2, 124, 240, 22, 17, 125, 16, 139, 142, 21, 138, 102, 84, 229, 143, 20, 52, 240, 19, 141, 158, 140,
    160, 155, 67, 176, 51, 118, 83, 120, 154, 119, 18, 80, 121, 159, 50, 66, 64, 48, 116, 156, 113, 117, 81, 157,
    82, 65, 134, 49, 135, 99, 115, 114, 98, 240, 129, 137, 133, 132, 97, 150, 240, 151, 131, 130, 96, 145, 112, 136,
    153, 149, 148, 147, 146, 128, 152, 144,
)


M0S = tuple(code % 16 for code in ORDER if STEPS[code // 16] == "M0")
BATCHES = ((0, 8), (8, 11), (11, 13), (13, 14), (14, 15), (15, 16))


def batch_of(chunk):
    at = M0S.index(chunk)
    return next(i for i, (first, last) in enumerate(BATCHES) if first <= at < last)


def kernel(
    slot_hbm, table_hbm, q_hbm, k_hbm, v_hbm, past_hbm, out,
    slot, table, qs, ks, vs, past, base, tally,
    qb, kb, vb, vt, q1, q2, q3, raised, kf, vf, vft, o_in, l_in, o_out, l_out, acc, top, tot, scores, ready, came,
    stage_sem, ex_send, q_ex, kv_ex, q_send, q_recv, kv_send, raised_recv, kf_recv, o_send, o_recv, f_send, f_recv,
):
    z = lax.axis_index("seq")
    n_z = lax.axis_size("seq")
    me = lax.axis_index("uly")
    y, x = me // 4, lax.rem(me, 4)
    below, above = z > 0, z < n_z - 1
    to_lower = {"seq": jnp.maximum(z - 1, 0)}
    to_upper = {"seq": jnp.minimum(z + 1, n_z - 1)}

    def peer(place):
        dy, dx = PLACES[place]
        return lax.rem(y + dy, 2) * 4 + lax.rem(x + dx, 4)

    def has(level):
        return z < n_z - level

    def columns_of(device, h):
        return pl.ds(pl.multiple_of((device * 2 + h) * HEAD_DIM, HEAD_DIM), HEAD_DIM)

    def place_rows(p):
        return pl.ds(p * 128, 128)

    barrier = pltpu.get_barrier_semaphore()
    for p in range(1, 8):
        pl.semaphore_signal(barrier, inc=1, device_id={"uly": peer(p)}, device_id_type=MESH)

    @pl.when(below)
    def _():
        pl.semaphore_signal(barrier, inc=1, device_id=to_lower, device_id_type=MESH)

    @pl.when(above)
    def _():
        for p in range(8):
            upper = {"seq": jnp.minimum(z + 1, n_z - 1), "uly": peer(p)}
            pl.semaphore_signal(barrier, inc=1, device_id=upper, device_id_type=MESH)

    gathered = ((q_hbm, qs, qb), (k_hbm, ks, kb), (v_hbm, vs, vb))

    def exchange_sem(t, h):
        return (q_ex if t == 0 else kv_ex).at[h]

    def own_copy(t, h):
        src, _staged, dst = gathered[t]
        return pltpu.make_async_copy(src.at[:, columns_of(me, h)], dst.at[h, place_rows(0)], exchange_sem(t, h))

    def exchange(t, h, p):
        _src, staged, dst = gathered[t]
        to = peer(MIRROR[p])
        return pltpu.make_async_remote_copy(
            src_ref=staged.at[:, columns_of(to, h)], dst_ref=dst.at[h, place_rows(p)],
            send_sem=ex_send.at[0], recv_sem=exchange_sem(t, h), device_id={"uly": to}, device_id_type=MESH,
        )

    def stage(t):
        return pltpu.make_async_copy(gathered[t][0], gathered[t][1], stage_sem.at[t])

    stored = [
        pltpu.make_async_copy(src, dst, stage_sem.at[3 + i])
        for i, (src, dst) in enumerate(((past_hbm, past), (slot_hbm, slot), (table_hbm, table)))
    ]
    for t in range(3):
        stage(t).start()
    for h in range(2):
        for t in range(3):
            own_copy(t, h).start()
    for copy in stored:
        copy.start()

    def no_parts():
        o_in[...] = jnp.zeros_like(o_in)
        l_in[...] = jnp.full_like(l_in, -1e30)
        kf[...] = jnp.zeros_like(kf)
        vf[...] = jnp.zeros_like(vf)

    def stored_sum():
        for copy in stored:
            copy.wait()
        coefs = [table[0, slot[i]] + table[1, slot[i]] for i in range(2)]

        def rows_sum(i, carry):
            rows = pl.ds(pl.multiple_of(i * 16, 16), 16)
            base[rows] = past[0, rows].astype(F32) * coefs[0] + past[1, rows].astype(F32) * coefs[1]
            return carry

        lax.fori_loop(0, 8, rows_sum, 0)

    pl.semaphore_wait(barrier, 7 + jnp.where(below, 8, 0) + jnp.where(above, 1, 0))

    blocks = (qb, q1, q2, q3)

    def split(chunk):
        return chunk // 8, place_rows(chunk % 8)

    def chunk_base(level):
        return 8 if level == 2 and MODES[0][1] < 3 else 0

    def query_sem(level, chunk):
        if level == 0:
            return o_recv.at[chunk]
        return q_recv.at[(level - 1) * 16 + chunk - chunk_base(level - 1)]

    def lower_piece(chunk):
        h, rows = split(chunk)
        to = peer(MIRROR[chunk % 8])
        return pltpu.make_async_remote_copy(
            src_ref=qs.at[:, columns_of(to, h)], dst_ref=q1.at[h, rows], send_sem=q_send.at[0],
            recv_sem=query_sem(1, chunk), device_id={"seq": jnp.maximum(z - 1, 0), "uly": to}, device_id_type=MESH,
        )

    def down(level, chunk):
        h, rows = split(chunk)
        return pltpu.make_async_remote_copy(
            src_ref=blocks[level].at[h, rows], dst_ref=blocks[level + 1].at[h, rows],
            send_sem=q_send.at[level], recv_sem=query_sem(level + 1, chunk), device_id=to_lower, device_id_type=MESH,
        )

    def raise_piece(t, p):
        _src, staged, _dst = gathered[t]
        dst = (None, kf, vf)[t].at[place_rows(0)] if p == 0 else raised.at[t - 1, p]
        return pltpu.make_async_remote_copy(
            src_ref=staged.at[:, columns_of(peer(p), RAISED)], dst_ref=dst, send_sem=kv_send,
            recv_sem=kf_recv if p == 0 else raised_recv.at[p], device_id=to_upper, device_id_type=MESH,
        )

    def pass_on(t, p):
        dst = (None, kf, vf)[t]
        return pltpu.make_async_remote_copy(
            src_ref=raised.at[t - 1, p], dst_ref=dst.at[place_rows(MIRROR[p])], send_sem=ex_send.at[1],
            recv_sem=kf_recv, device_id={"uly": peer(p)}, device_id_type=MESH,
        )

    def up(level, chunk):
        return [
            pltpu.make_async_remote_copy(
                src_ref=src.at[level, chunk], dst_ref=dst.at[level, chunk],
                send_sem=o_send.at[level], recv_sem=query_sem(level, chunk), device_id=to_upper, device_id_type=MESH,
            )
            for src, dst in ((o_out, o_in), (l_out, l_in))
        ]

    def arrived(semaphore, count):
        pltpu.make_async_copy(tally.at[pl.ds(0, count)], tally.at[pl.ds(0, count)], semaphore).wait()

    def finish(chunk):
        h, rows = split(chunk)
        place = chunk % 8
        return pltpu.make_async_remote_copy(
            src_ref=ready.at[h, rows], dst_ref=came.at[MIRROR[place], h], send_sem=f_send,
            recv_sem=f_recv.at[batch_of(chunk)], device_id={"uly": peer(place)}, device_id_type=MESH,
        )

    done = set()

    def expect(*wanted):
        by_condition = {}
        for condition, key, copies in wanted:
            if key not in done:
                done.add(key)
                by_condition.setdefault(id(condition), (condition, []))[1].extend(copies)
        for condition, copies in by_condition.values():

            def wait(copies=copies):
                for copy in copies:
                    copy()

            if condition is None:
                wait()
            else:
                pl.when(condition)(wait)

    exists = [None, has(1), has(2), has(3)]
    came_up = [below, has(1) & below, has(2) & below]

    def queries(level, chunk):
        if level == 0:
            h = chunk // 8
            return (None, ("own", h), [functools.partial(arrived, q_ex.at[h], 512)])
        return (exists[level], ("down", level, chunk), [functools.partial(arrived, query_sem(level, chunk), 64)])

    def part(level, chunk):
        return (came_up[level], ("up", level, chunk), [functools.partial(arrived, query_sem(level, chunk), 65)])

    def in_vmem(t):
        return (None, ("in_vmem", t), [lambda: stage(t).wait()])

    def first_stage(step, pair, buffer):
        level = int(step[1])
        h, rows = pair // 4, pl.ds((pair % 4) * 256, 256)
        source = blocks[level]
        if level == 3 and h == RAISED:
            source = q2
        query = source[h, rows]
        tops = []
        for b in range(4):
            of_keys = pl.ds(b * 256, 256)
            keys = kf[of_keys] if level == 3 and h == RAISED else kb[h, of_keys]
            s = lax.dot_general(keys, query, NT, preferred_element_type=F32)
            if level == 0:
                key_row = lax.broadcasted_iota(jnp.int32, (256, 1), 0)
                query_row = lax.broadcasted_iota(jnp.int32, (1, 256), 1)
                key_pos = jnp.where(key_row < 128, peer(2 * b) * 128, peer(2 * b + 1) * 128 - 128) + key_row
                first = 2 * (pair % 4)
                query_pos = jnp.where(query_row < 128, peer(first) * 128, peer(first + 1) * 128 - 128) + query_row
                s = jnp.where(key_pos <= query_pos, s, -1e30)
            scores[buffer, pl.ds(b * 256, 256)] = s
            tops.append(jnp.max(s.reshape(32, 8, 256), axis=0))
        tops = jnp.maximum(jnp.maximum(tops[0], tops[1]), jnp.maximum(tops[2], tops[3]))
        return jnp.max(tops, axis=0, keepdims=True)

    def second_stage(step, pair, buffer, highest):
        level = int(step[1])
        h = pair // 4
        total = jnp.zeros((8, 256), F32)
        weighted = None
        for b in range(4):
            prob = jnp.exp2((scores[buffer, pl.ds(b * 256, 256)] - highest) * SCALE)
            total += jnp.sum(prob.reshape(32, 8, 256), axis=0)
            of_keys = pl.ds(b * 256, 256)
            values = vft[:, of_keys] if level == 3 and h == RAISED else vt[h, :, of_keys]
            term = lax.dot_general(values, prob.astype(BF16), NN, preferred_element_type=F32)
            weighted = term if weighted is None else weighted + term
        return weighted, jnp.sum(total, axis=0, keepdims=True)

    pending = []
    turn = [0]

    def advance(step=None, pair=None):
        last = pending.pop() if pending else None
        if step is not None:
            buffer = turn[0] % 2
            turn[0] += 1
            level = int(step[1])
            highest = first_stage(step, pair, buffer)
        if last is not None:
            old_step, old_pair, old_buffer = last
            old = int(old_step[1])
            old_top = top[old, old_pair]
            weighted, total = second_stage(old_step, old_pair, old_buffer, old_top)
            if old == 3 and MODES[old_pair // 4][1] == 3:
                mean = (weighted / total).astype(BF16)
                log_total = old_top * SCALE + jnp.log2(total)
                for i in range(2):
                    o_out[2, 2 * old_pair + i] = mean[:, i * 128 : i * 128 + 128]
                    l_out[2, 2 * old_pair + i] = log_total[:, i * 128 : i * 128 + 128]
            else:
                acc[old, old_pair] = weighted
                tot[old, old_pair] = total
                if old == 3:
                    top[old, old_pair] = jnp.where(below, old_top, -1e30)
        if step is not None:
            top[level, pair] = highest
            pending.append((step, pair, buffer))
        if last is not None and old == 3 and MODES[old_pair // 4][1] == 3:

            @pl.when(has(3))
            def _():
                for i in range(2):
                    for copy in up(2, 2 * old_pair + i):
                        copy.start()

    def settle(*units):
        if pending and pending[0][:2] in units:
            advance()

    def merged(chunk, level):
        pair, lanes = chunk // 2, slice(chunk % 2 * 128, chunk % 2 * 128 + 128)
        own = top[level, pair][:, lanes] * SCALE
        if level == 2 and MODES[chunk // 8][0] == 1:
            new = top[3, pair][:, lanes] * SCALE
            new_total, new_weighted = tot[3, pair][:, lanes], acc[3, pair, :, lanes]
        else:
            new = l_in[level, chunk]
            new_total, new_weighted = 1.0, o_in[level, chunk].astype(F32)
        most = jnp.maximum(own, new)
        a, b = jnp.exp2(own - most), jnp.exp2(new - most)
        total = tot[level, pair][:, lanes] * a + new_total * b
        weighted = acc[level, pair, :, lanes] * a + new_weighted * b
        return weighted / total, most + jnp.log2(total)

    def run(step, which):
        if step == "S0":
            expect(in_vmem(0))
            pl.when(below)(lower_piece(which).start)
        elif step in ("R1", "R2"):
            level = int(step[1])
            expect(queries(level, which))
            pl.when(has(level) & below)(down(level, which).start)
        elif step == "FL":
            advance()
        elif step == "XI":
            for code in EXCHANGE[which * 7 : which * 7 + 7]:
                expect(in_vmem(code // 16))
                exchange(code // 16, code // 8 % 2, code % 8).start()
        elif step == "SK":
            expect(in_vmem(1), in_vmem(2))

            @pl.when(above)
            def _():
                for t in (1, 2):
                    raise_piece(t, which).start()
        elif step == "XK":
            expect((below, ("raised", which), [functools.partial(arrived, raised_recv.at[which], 128)]))

            @pl.when(below)
            def _():
                for t in (1, 2):
                    pass_on(t, which).start()
        elif step == "KV":
            expect((None, ("keys", which), [functools.partial(arrived, kv_ex.at[which], 1024)]))
            vt[which] = jnp.transpose(vb[which])
        elif step == "KF":
            expect((below, ("raised",), [functools.partial(arrived, kf_recv, 1024)]))
            vft[...] = jnp.transpose(vf[...])
        elif step[0] == "C":
            level = int(step[1])
            if level == 3 and MODES[which // 4][0] == 1:
                level = 2
            expect(queries(level, 2 * which), queries(level, 2 * which + 1))
            advance(step, which)
        elif step == "M0":
            settle(("C0", which // 2))
            expect(part(0, which))
            mean, _unused = merged(which, 0)
            h, rows = split(which)
            if which % 8 == 0:
                came[0, h] = jnp.transpose(mean).astype(BF16)
            else:
                ready[h, rows] = jnp.transpose(mean).astype(BF16)
                finish(which).start()
        else:
            level = int(step[1])
            if level == 2 and MODES[which // 8][0] == 1:
                settle(("C2", which // 2), ("C3", which // 2))
            else:
                settle((f"C{level}", which // 2))
                expect(part(level, which))
            mean, log_total = merged(which, level)
            o_out[level - 1, which] = mean.astype(BF16)
            l_out[level - 1, which] = log_total

            @pl.when(has(level))
            def _(level=level, which=which):
                for copy in up(level - 1, which):
                    copy.start()

    summed = False
    for code in ORDER:
        step, which = STEPS[code // 16], code % 16
        if not summed and step not in ("XI", "SK", "S0"):
            pl.when(z == 0)(no_parts)
            stored_sum()
            summed = True
        run(step, which)

    for batch, (first, last) in enumerate(BATCHES):
        chunks = M0S[first:last]
        remote = sum(1 for chunk in chunks if chunk % 8)
        if remote:
            arrived(f_recv.at[batch], remote * 64)
        for chunk in chunks:
            h, place = chunk // 8, MIRROR[chunk % 8]
            lanes = columns_of(peer(place), h)
            out[:, lanes] = (base[:, lanes] + came[place, h].astype(F32)).astype(BF16)

    sent = scores.at[:, pl.ds(0, 672)]
    pltpu.make_async_copy(sent, sent, ex_send.at[0]).wait()
    sent = ready.at[:, pl.ds(0, 896)]
    pltpu.make_async_copy(sent, sent, f_send).wait()
    pl.when(below)(functools.partial(arrived, ex_send.at[1], 896))
    pl.when(above)(functools.partial(arrived, kv_send, 1024))
    for level in range(3):
        heads = sum(1 for _up_hops, down_hops in MODES if down_hops > level)
        pl.when(has(level) & below)(functools.partial(arrived, q_send.at[level], 512 * heads))
        pl.when(has(level + 1))(functools.partial(arrived, o_send.at[level], 520 * heads))


def attention(slot, table, queries, keys, values, past):
    block = pltpu.VMEM((2, 1024, HEAD_DIM), BF16)
    turned = pltpu.VMEM((2, HEAD_DIM, 1024), BF16)
    staged = pltpu.VMEM(queries.shape, BF16)
    parts, logs = (3, 16, HEAD_DIM, 128), (3, 16, 1, 128)
    dma = pltpu.SemaphoreType.DMA
    chunks = 32 + 8 * sum(1 for _up_hops, down_hops in MODES if down_hops == 3)
    return pl.pallas_call(
        kernel,
        out_shape=pltpu.VMEM(queries.shape, BF16),
        in_specs=[pl.BlockSpec(memory_space=pl.ANY)] * 6,
        scratch_shapes=[
            pltpu.SMEM(slot.shape, jnp.int32), pltpu.SMEM(table.shape, F32), staged, staged, staged,
            pltpu.VMEM(past.shape, BF16), pltpu.VMEM(queries.shape, F32), pltpu.VMEM((1040, 1, 128), F32),
            block, block, block, turned, block, block, block, pltpu.VMEM((2, 8, 128, HEAD_DIM), BF16),
            pltpu.VMEM((1024, HEAD_DIM), BF16), pltpu.VMEM((1024, HEAD_DIM), BF16), pltpu.VMEM((HEAD_DIM, 1024), BF16),
            pltpu.VMEM(parts, BF16), pltpu.VMEM(logs, F32), pltpu.VMEM(parts, BF16), pltpu.VMEM(logs, F32),
            pltpu.VMEM((4, 8, HEAD_DIM, 256), F32), pltpu.VMEM((4, 8, 1, 256), F32), pltpu.VMEM((4, 8, 1, 256), F32),
            pltpu.VMEM((2, 1024, 256), F32), block, pltpu.VMEM((8, 2, 128, HEAD_DIM), BF16),
            dma((6,)), dma((2,)), dma((2,)), dma((2,)), dma((3,)), dma((chunks,)), dma(()), dma((8,)), dma(()),
            dma((3,)), dma((16,)), dma(()), dma((len(BATCHES),)),
        ],
        compiler_params=pltpu.CompilerParams(collective_id=0, has_side_effects=True),
        name="attention",
    )(slot, table, queries, keys, values, past)


def shards(queries, keys, values, past_outputs, dwa_slot, dwa_table):
    return attention(dwa_slot, dwa_table, queries, keys, values, past_outputs)


def solution(mesh):
    tokens = P(("rep", "seq", "uly"), None)
    return jax.shard_map(
        shards,
        mesh=mesh,
        in_specs=(tokens, tokens, tokens, P(None, ("rep", "seq", "uly"), None), P(), P()),
        out_specs=tokens,
        check_vma=False,
    )
```

```python
import functools
import math

import jax
import jax.numpy as jnp
from jax import lax
from jax.experimental import pallas as pl
from jax.experimental.pallas import tpu as pltpu
from jax.sharding import PartitionSpec as P

MESH = pl.DeviceIdType.MESH
HEAD_DIM = 128
SCALE = math.log2(math.e) / math.sqrt(HEAD_DIM)
BF16, F32 = jnp.bfloat16, jnp.float32
NT = (((1,), (1,)), ((), ()))
NN = (((1,), (0,)), ((), ()))

PLACES = ((0, 0), (0, 1), (0, 3), (1, 0), (1, 1), (1, 3), (0, 2), (1, 2))
MIRROR = tuple(PLACES.index((dy, (4 - dx) % 4)) for dy, dx in PLACES)

MODES = ((1, 2), (0, 3))
RAISED = next(h for h, (up_hops, _down_hops) in enumerate(MODES) if up_hops)
EXCHANGE = (
    25, 26, 27, 28, 29, 30, 31, 41, 42, 43, 44, 45, 46, 47, 9, 10, 11, 12, 13, 14, 15, 17, 18, 19,
    20, 21, 22, 23, 33, 34, 35, 36, 37, 38, 39, 1, 2, 3, 4, 5, 6, 7,
)

STEPS = ("S0", "R1", "R2", "C3", "C2", "C1", "C0", "M2", "M1", "M0", "KV", "KF", "SK", "XK", "XI", "FL")
ORDER = (
    15, 196, 199, 195, 11, 197, 198, 192, 194, 10, 14, 12, 13, 8, 9, 224, 225, 226, 27, 26, 31, 30, 212, 28,
    193, 29, 43, 214, 213, 42, 47, 46, 215, 161, 44, 69, 45, 24, 71, 1, 211, 25, 7, 5, 6, 0, 85, 4,
    227, 53, 240, 55, 240, 54, 240, 122, 228, 3, 86, 210, 70, 123, 240, 126, 209, 40, 103, 68, 41, 100, 127, 101,
    87, 23, 2, 124, 240, 22, 17, 125, 16, 139, 142, 21, 138, 102, 84, 229, 143, 20, 52, 240, 19, 141, 158, 140,
    160, 155, 67, 176, 51, 118, 83, 120, 154, 119, 18, 80, 121, 159, 50, 66, 64, 48, 116, 156, 113, 117, 81, 157,
    82, 65, 134, 49, 135, 99, 115, 114, 98, 240, 129, 137, 133, 132, 97, 150, 240, 151, 131, 130, 96, 145, 112, 136,
    153, 149, 148, 147, 146, 128, 152, 144,
)


PAUSES = {STEPS.index("M2") * 16 + 10: 2000}

M0S = tuple(code % 16 for code in ORDER if STEPS[code // 16] == "M0")
BATCHES = ((0, 8), (8, 11), (11, 13), (13, 14), (14, 15), (15, 16))


def batch_of(chunk):
    at = M0S.index(chunk)
    return next(i for i, (first, last) in enumerate(BATCHES) if first <= at < last)


def kernel(
    slot_hbm, table_hbm, q_hbm, k_hbm, v_hbm, past_hbm, out,
    slot, table, qs, ks, vs, past, base, tally,
    qb, kb, vb, vt, q1, q2, q3, raised, kf, vf, vft, o_in, l_in, o_out, l_out, acc, top, tot, scores, ready, came,
    stage_sem, ex_send, q_ex, kv_ex, q_send, q_recv, kv_send, raised_recv, kf_recv, o_send, o_recv, f_send, f_recv,
):
    z = lax.axis_index("seq")
    n_z = lax.axis_size("seq")
    me = lax.axis_index("uly")
    y, x = me // 4, lax.rem(me, 4)
    below, above = z > 0, z < n_z - 1
    to_lower = {"seq": jnp.maximum(z - 1, 0)}
    to_upper = {"seq": jnp.minimum(z + 1, n_z - 1)}

    def peer(place):
        dy, dx = PLACES[place]
        return lax.rem(y + dy, 2) * 4 + lax.rem(x + dx, 4)

    def has(level):
        return z < n_z - level

    def columns_of(device, h):
        return pl.ds(pl.multiple_of((device * 2 + h) * HEAD_DIM, HEAD_DIM), HEAD_DIM)

    def place_rows(p):
        return pl.ds(p * 128, 128)

    barrier = pltpu.get_barrier_semaphore()
    for p in range(1, 8):
        pl.semaphore_signal(barrier, inc=1, device_id={"uly": peer(p)}, device_id_type=MESH)

    @pl.when(below)
    def _():
        pl.semaphore_signal(barrier, inc=1, device_id=to_lower, device_id_type=MESH)

    @pl.when(above)
    def _():
        for p in range(8):
            upper = {"seq": jnp.minimum(z + 1, n_z - 1), "uly": peer(p)}
            pl.semaphore_signal(barrier, inc=1, device_id=upper, device_id_type=MESH)

    gathered = ((q_hbm, qs, qb), (k_hbm, ks, kb), (v_hbm, vs, vb))

    def exchange_sem(t, h):
        return (q_ex if t == 0 else kv_ex).at[h]

    def own_copy(t, h):
        src, _staged, dst = gathered[t]
        return pltpu.make_async_copy(src.at[:, columns_of(me, h)], dst.at[h, place_rows(0)], exchange_sem(t, h))

    def exchange(t, h, p):
        _src, staged, dst = gathered[t]
        to = peer(MIRROR[p])
        return pltpu.make_async_remote_copy(
            src_ref=staged.at[:, columns_of(to, h)], dst_ref=dst.at[h, place_rows(p)],
            send_sem=ex_send.at[0], recv_sem=exchange_sem(t, h), device_id={"uly": to}, device_id_type=MESH,
        )

    def stage(t):
        return pltpu.make_async_copy(gathered[t][0], gathered[t][1], stage_sem.at[t])

    stored = [
        pltpu.make_async_copy(src, dst, stage_sem.at[3 + i])
        for i, (src, dst) in enumerate(((past_hbm, past), (slot_hbm, slot), (table_hbm, table)))
    ]
    for t in range(3):
        stage(t).start()
    for h in range(2):
        for t in range(3):
            own_copy(t, h).start()
    for copy in stored:
        copy.start()

    def no_parts():
        o_in[...] = jnp.zeros_like(o_in)
        l_in[...] = jnp.full_like(l_in, -1e30)
        kf[...] = jnp.zeros_like(kf)
        vf[...] = jnp.zeros_like(vf)

    def stored_sum():
        for copy in stored:
            copy.wait()
        coefs = [table[0, slot[i]] + table[1, slot[i]] for i in range(2)]

        def rows_sum(i, carry):
            rows = pl.ds(pl.multiple_of(i * 16, 16), 16)
            base[rows] = past[0, rows].astype(F32) * coefs[0] + past[1, rows].astype(F32) * coefs[1]
            return carry

        lax.fori_loop(0, 8, rows_sum, 0)

    pl.semaphore_wait(barrier, 7 + jnp.where(below, 8, 0) + jnp.where(above, 1, 0))

    blocks = (qb, q1, q2, q3)

    def split(chunk):
        return chunk // 8, place_rows(chunk % 8)

    def chunk_base(level):
        return 8 if level == 2 and MODES[0][1] < 3 else 0

    def query_sem(level, chunk):
        if level == 0:
            return o_recv.at[chunk]
        return q_recv.at[(level - 1) * 16 + chunk - chunk_base(level - 1)]

    def lower_piece(chunk):
        h, rows = split(chunk)
        to = peer(MIRROR[chunk % 8])
        return pltpu.make_async_remote_copy(
            src_ref=qs.at[:, columns_of(to, h)], dst_ref=q1.at[h, rows], send_sem=q_send.at[0],
            recv_sem=query_sem(1, chunk), device_id={"seq": jnp.maximum(z - 1, 0), "uly": to}, device_id_type=MESH,
        )

    def down(level, chunk):
        h, rows = split(chunk)
        return pltpu.make_async_remote_copy(
            src_ref=blocks[level].at[h, rows], dst_ref=blocks[level + 1].at[h, rows],
            send_sem=q_send.at[level], recv_sem=query_sem(level + 1, chunk), device_id=to_lower, device_id_type=MESH,
        )

    def raise_piece(t, p):
        _src, staged, _dst = gathered[t]
        dst = (None, kf, vf)[t].at[place_rows(0)] if p == 0 else raised.at[t - 1, p]
        return pltpu.make_async_remote_copy(
            src_ref=staged.at[:, columns_of(peer(p), RAISED)], dst_ref=dst, send_sem=kv_send,
            recv_sem=kf_recv if p == 0 else raised_recv.at[p], device_id=to_upper, device_id_type=MESH,
        )

    def pass_on(t, p):
        dst = (None, kf, vf)[t]
        return pltpu.make_async_remote_copy(
            src_ref=raised.at[t - 1, p], dst_ref=dst.at[place_rows(MIRROR[p])], send_sem=ex_send.at[1],
            recv_sem=kf_recv, device_id={"uly": peer(p)}, device_id_type=MESH,
        )

    def up(level, chunk):
        return [
            pltpu.make_async_remote_copy(
                src_ref=src.at[level, chunk], dst_ref=dst.at[level, chunk],
                send_sem=o_send.at[level], recv_sem=query_sem(level, chunk), device_id=to_upper, device_id_type=MESH,
            )
            for src, dst in ((o_out, o_in), (l_out, l_in))
        ]

    def arrived(semaphore, count):
        pltpu.make_async_copy(tally.at[pl.ds(0, count)], tally.at[pl.ds(0, count)], semaphore).wait()

    def finish(chunk):
        h, rows = split(chunk)
        place = chunk % 8
        return pltpu.make_async_remote_copy(
            src_ref=ready.at[h, rows], dst_ref=came.at[MIRROR[place], h], send_sem=f_send,
            recv_sem=f_recv.at[batch_of(chunk)], device_id={"uly": peer(place)}, device_id_type=MESH,
        )

    done = set()

    def expect(*wanted):
        by_condition = {}
        for condition, key, copies in wanted:
            if key not in done:
                done.add(key)
                by_condition.setdefault(id(condition), (condition, []))[1].extend(copies)
        for condition, copies in by_condition.values():

            def wait(copies=copies):
                for copy in copies:
                    copy()

            if condition is None:
                wait()
            else:
                pl.when(condition)(wait)

    exists = [None, has(1), has(2), has(3)]
    came_up = [below, has(1) & below, has(2) & below]

    def queries(level, chunk):
        if level == 0:
            h = chunk // 8
            return (None, ("own", h), [functools.partial(arrived, q_ex.at[h], 512)])
        return (exists[level], ("down", level, chunk), [functools.partial(arrived, query_sem(level, chunk), 64)])

    def part(level, chunk):
        return (came_up[level], ("up", level, chunk), [functools.partial(arrived, query_sem(level, chunk), 65)])

    def in_vmem(t):
        return (None, ("in_vmem", t), [lambda: stage(t).wait()])

    def first_stage(step, pair, buffer):
        level = int(step[1])
        h, rows = pair // 4, pl.ds((pair % 4) * 256, 256)
        source = blocks[level]
        if level == 3 and h == RAISED:
            source = q2
        query = source[h, rows]
        tops = []
        for b in range(4):
            of_keys = pl.ds(b * 256, 256)
            keys = kf[of_keys] if level == 3 and h == RAISED else kb[h, of_keys]
            s = lax.dot_general(keys, query, NT, preferred_element_type=F32)
            if level == 0:
                key_row = lax.broadcasted_iota(jnp.int32, (256, 1), 0)
                query_row = lax.broadcasted_iota(jnp.int32, (1, 256), 1)
                key_pos = jnp.where(key_row < 128, peer(2 * b) * 128, peer(2 * b + 1) * 128 - 128) + key_row
                first = 2 * (pair % 4)
                query_pos = jnp.where(query_row < 128, peer(first) * 128, peer(first + 1) * 128 - 128) + query_row
                s = jnp.where(key_pos <= query_pos, s, -1e30)
            scores[buffer, pl.ds(b * 256, 256)] = s
            tops.append(jnp.max(s.reshape(32, 8, 256), axis=0))
        tops = jnp.maximum(jnp.maximum(tops[0], tops[1]), jnp.maximum(tops[2], tops[3]))
        return jnp.max(tops, axis=0, keepdims=True)

    def second_stage(step, pair, buffer, highest):
        level = int(step[1])
        h = pair // 4
        total = jnp.zeros((8, 256), F32)
        weighted = None
        for b in range(4):
            prob = jnp.exp2((scores[buffer, pl.ds(b * 256, 256)] - highest) * SCALE)
            total += jnp.sum(prob.reshape(32, 8, 256), axis=0)
            of_keys = pl.ds(b * 256, 256)
            values = vft[:, of_keys] if level == 3 and h == RAISED else vt[h, :, of_keys]
            term = lax.dot_general(values, prob.astype(BF16), NN, preferred_element_type=F32)
            weighted = term if weighted is None else weighted + term
        return weighted, jnp.sum(total, axis=0, keepdims=True)

    pending = []
    turn = [0]

    def advance(step=None, pair=None):
        last = pending.pop() if pending else None
        if step is not None:
            buffer = turn[0] % 2
            turn[0] += 1
            level = int(step[1])
            highest = first_stage(step, pair, buffer)
        if last is not None:
            old_step, old_pair, old_buffer = last
            old = int(old_step[1])
            old_top = top[old, old_pair]
            weighted, total = second_stage(old_step, old_pair, old_buffer, old_top)
            if old == 3 and MODES[old_pair // 4][1] == 3:
                mean = (weighted / total).astype(BF16)
                log_total = old_top * SCALE + jnp.log2(total)
                for i in range(2):
                    o_out[2, 2 * old_pair + i] = mean[:, i * 128 : i * 128 + 128]
                    l_out[2, 2 * old_pair + i] = log_total[:, i * 128 : i * 128 + 128]
            else:
                acc[old, old_pair] = weighted
                tot[old, old_pair] = total
                if old == 3:
                    top[old, old_pair] = jnp.where(below, old_top, -1e30)
        if step is not None:
            top[level, pair] = highest
            pending.append((step, pair, buffer))
        if last is not None and old == 3 and MODES[old_pair // 4][1] == 3:

            @pl.when(has(3))
            def _():
                for i in range(2):
                    for copy in up(2, 2 * old_pair + i):
                        copy.start()

    def settle(*units):
        if pending and pending[0][:2] in units:
            advance()

    def merged(chunk, level):
        pair, lanes = chunk // 2, slice(chunk % 2 * 128, chunk % 2 * 128 + 128)
        own = top[level, pair][:, lanes] * SCALE
        if level == 2 and MODES[chunk // 8][0] == 1:
            new = top[3, pair][:, lanes] * SCALE
            new_total, new_weighted = tot[3, pair][:, lanes], acc[3, pair, :, lanes]
        else:
            new = l_in[level, chunk]
            new_total, new_weighted = 1.0, o_in[level, chunk].astype(F32)
        most = jnp.maximum(own, new)
        a, b = jnp.exp2(own - most), jnp.exp2(new - most)
        total = tot[level, pair][:, lanes] * a + new_total * b
        weighted = acc[level, pair, :, lanes] * a + new_weighted * b
        return weighted / total, most + jnp.log2(total)

    def run(step, which):
        if step == "S0":
            expect(in_vmem(0))
            pl.when(below)(lower_piece(which).start)
        elif step in ("R1", "R2"):
            level = int(step[1])
            expect(queries(level, which))
            pl.when(has(level) & below)(down(level, which).start)
        elif step == "FL":
            advance()
        elif step == "XI":
            for code in EXCHANGE[which * 7 : which * 7 + 7]:
                expect(in_vmem(code // 16))
                exchange(code // 16, code // 8 % 2, code % 8).start()
        elif step == "SK":
            expect(in_vmem(1), in_vmem(2))

            @pl.when(above)
            def _():
                for t in (1, 2):
                    raise_piece(t, which).start()
        elif step == "XK":
            expect((below, ("raised", which), [functools.partial(arrived, raised_recv.at[which], 128)]))

            @pl.when(below)
            def _():
                for t in (1, 2):
                    pass_on(t, which).start()
        elif step == "KV":
            expect((None, ("keys", which), [functools.partial(arrived, kv_ex.at[which], 1024)]))
            vt[which] = jnp.transpose(vb[which])
        elif step == "KF":
            expect((below, ("raised",), [functools.partial(arrived, kf_recv, 1024)]))
            vft[...] = jnp.transpose(vf[...])
        elif step[0] == "C":
            level = int(step[1])
            if level == 3 and MODES[which // 4][0] == 1:
                level = 2
            expect(queries(level, 2 * which), queries(level, 2 * which + 1))
            advance(step, which)
        elif step == "M0":
            settle(("C0", which // 2))
            expect(part(0, which))
            mean, _unused = merged(which, 0)
            h, rows = split(which)
            if which % 8 == 0:
                came[0, h] = jnp.transpose(mean).astype(BF16)
            else:
                ready[h, rows] = jnp.transpose(mean).astype(BF16)
                finish(which).start()
        else:
            level = int(step[1])
            if level == 2 and MODES[which // 8][0] == 1:
                settle(("C2", which // 2), ("C3", which // 2))
            else:
                settle((f"C{level}", which // 2))
                expect(part(level, which))
            mean, log_total = merged(which, level)
            o_out[level - 1, which] = mean.astype(BF16)
            l_out[level - 1, which] = log_total

            @pl.when(has(level))
            def _(level=level, which=which):
                for copy in up(level - 1, which):
                    copy.start()

    summed = False
    for code in ORDER:
        step, which = STEPS[code // 16], code % 16
        if not summed and step not in ("XI", "SK", "S0"):
            pl.when(z == 0)(no_parts)
            stored_sum()
            summed = True
        ns = PAUSES.get(code)
        if ns:
            pl.when(lax.rem(lax.axis_index("rep"), 2) == 1)(functools.partial(pl.delay, ns))
        run(step, which)

    for batch, (first, last) in enumerate(BATCHES):
        chunks = M0S[first:last]
        remote = sum(1 for chunk in chunks if chunk % 8)
        if remote:
            arrived(f_recv.at[batch], remote * 64)
        for chunk in chunks:
            h, place = chunk // 8, MIRROR[chunk % 8]
            lanes = columns_of(peer(place), h)
            out[:, lanes] = (base[:, lanes] + came[place, h].astype(F32)).astype(BF16)

    sent = scores.at[:, pl.ds(0, 672)]
    pltpu.make_async_copy(sent, sent, ex_send.at[0]).wait()
    sent = ready.at[:, pl.ds(0, 896)]
    pltpu.make_async_copy(sent, sent, f_send).wait()
    pl.when(below)(functools.partial(arrived, ex_send.at[1], 896))
    pl.when(above)(functools.partial(arrived, kv_send, 1024))
    for level in range(3):
        heads = sum(1 for _up_hops, down_hops in MODES if down_hops > level)
        pl.when(has(level) & below)(functools.partial(arrived, q_send.at[level], 512 * heads))
        pl.when(has(level + 1))(functools.partial(arrived, o_send.at[level], 520 * heads))


def attention(slot, table, queries, keys, values, past):
    block = pltpu.VMEM((2, 1024, HEAD_DIM), BF16)
    turned = pltpu.VMEM((2, HEAD_DIM, 1024), BF16)
    staged = pltpu.VMEM(queries.shape, BF16)
    parts, logs = (3, 16, HEAD_DIM, 128), (3, 16, 1, 128)
    dma = pltpu.SemaphoreType.DMA
    chunks = 32 + 8 * sum(1 for _up_hops, down_hops in MODES if down_hops == 3)
    return pl.pallas_call(
        kernel,
        out_shape=pltpu.VMEM(queries.shape, BF16),
        in_specs=[pl.BlockSpec(memory_space=pl.ANY)] * 6,
        scratch_shapes=[
            pltpu.SMEM(slot.shape, jnp.int32), pltpu.SMEM(table.shape, F32), staged, staged, staged,
            pltpu.VMEM(past.shape, BF16), pltpu.VMEM(queries.shape, F32), pltpu.VMEM((1040, 1, 128), F32),
            block, block, block, turned, block, block, block, pltpu.VMEM((2, 8, 128, HEAD_DIM), BF16),
            pltpu.VMEM((1024, HEAD_DIM), BF16), pltpu.VMEM((1024, HEAD_DIM), BF16), pltpu.VMEM((HEAD_DIM, 1024), BF16),
            pltpu.VMEM(parts, BF16), pltpu.VMEM(logs, F32), pltpu.VMEM(parts, BF16), pltpu.VMEM(logs, F32),
            pltpu.VMEM((4, 8, HEAD_DIM, 256), F32), pltpu.VMEM((4, 8, 1, 256), F32), pltpu.VMEM((4, 8, 1, 256), F32),
            pltpu.VMEM((2, 1024, 256), F32), block, pltpu.VMEM((8, 2, 128, HEAD_DIM), BF16),
            dma((6,)), dma((2,)), dma((2,)), dma((2,)), dma((3,)), dma((chunks,)), dma(()), dma((8,)), dma(()),
            dma((3,)), dma((16,)), dma(()), dma((len(BATCHES),)),
        ],
        compiler_params=pltpu.CompilerParams(collective_id=0, has_side_effects=True),
        name="attention",
    )(slot, table, queries, keys, values, past)


def shards(queries, keys, values, past_outputs, dwa_slot, dwa_table):
    return attention(dwa_slot, dwa_table, queries, keys, values, past_outputs)


def solution(mesh):
    tokens = P(("rep", "seq", "uly"), None)
    return jax.shard_map(
        shards,
        mesh=mesh,
        in_specs=(tokens, tokens, tokens, P(None, ("rep", "seq", "uly"), None), P(), P()),
        out_specs=tokens,
        check_vma=False,
    )
```

```python
import functools
import math

import jax
import jax.numpy as jnp
from jax import lax
from jax.experimental import pallas as pl
from jax.experimental.pallas import tpu as pltpu
from jax.sharding import PartitionSpec as P

MESH = pl.DeviceIdType.MESH
HEAD_DIM = 128
SCALE = math.log2(math.e) / math.sqrt(HEAD_DIM)
BF16, F32 = jnp.bfloat16, jnp.float32
NT = (((1,), (1,)), ((), ()))
NN = (((1,), (0,)), ((), ()))

PLACES = ((0, 0), (0, 1), (0, 3), (1, 0), (1, 1), (1, 3), (0, 2), (1, 2))
MIRROR = tuple(PLACES.index((dy, (4 - dx) % 4)) for dy, dx in PLACES)

MODES = ((1, 2), (0, 3))
RAISED = next(h for h, (up_hops, _down_hops) in enumerate(MODES) if up_hops)
EXCHANGE = (
    25, 26, 27, 28, 29, 30, 31, 41, 42, 43, 44, 45, 46, 47, 17, 18, 19, 20, 21, 22, 23, 33, 34, 35,
    36, 37, 38, 39, 9, 10, 11, 12, 13, 14, 15, 1, 2, 3, 4, 5, 6, 7,
)

STEPS = ("S0", "R1", "R2", "C3", "C2", "C1", "C0", "M2", "M1", "M0", "KV", "KF", "SK", "XK", "XI", "FL")
DIRECT = (1, 2, 3, 9)
ORDER = (
    12, 192, 13, 197, 199, 196, 15, 195, 193, 11, 194, 10, 14, 198, 9, 224, 225, 226, 28, 29, 27, 26, 31, 215,
    30, 212, 44, 45, 43, 42, 210, 47, 46, 6, 7, 8, 4, 25, 161, 0, 5, 209, 69, 70, 227, 54, 240, 53,
    240, 55, 240, 124, 1, 213, 86, 2, 240, 122, 214, 24, 3, 125, 22, 71, 87, 84, 23, 85, 211, 123, 228, 126,
    20, 240, 140, 21, 127, 141, 160, 40, 138, 68, 41, 80, 16, 17, 142, 83, 82, 139, 67, 176, 18, 143, 51, 119,
    229, 118, 19, 66, 50, 116, 81, 117, 52, 101, 103, 154, 135, 159, 134, 102, 155, 158, 48, 65, 156, 133, 157, 132,
    49, 64, 113, 121, 114, 99, 98, 151, 150, 120, 115, 100, 149, 96, 240, 129, 112, 137, 148, 130, 131, 97, 136, 240,
    145, 128, 146, 153, 147, 152, 144,
)


PAUSES = {STEPS.index("M2") * 16 + 12: 2000}
LATE_PAUSES = {STEPS.index("M2") * 16 + 12: 2000}

M0S = tuple(code % 16 for code in ORDER if STEPS[code // 16] == "M0" and code % 16 not in DIRECT)
BATCHES = ((0, 8), (8, len(M0S) - 2), (len(M0S) - 2, len(M0S) - 1), (len(M0S) - 1, len(M0S)))


def batch_of(chunk):
    at = M0S.index(chunk)
    return next(i for i, (first, last) in enumerate(BATCHES) if first <= at < last)


def kernel(
    slot_hbm, table_hbm, q_hbm, k_hbm, v_hbm, past_hbm, out,
    slot, table, qs, ks, vs, past, base, tally,
    qb, kb, vb, vt, q1, q2, q3, raised, kf, vf, vft, o_in, l_in, o_out, l_out, acc, top, tot, scores, ready, came,
    part_out, part_log_out, part_in, part_log_in,
    stage_sem, ex_send, q_ex, kv_ex, q_send, q_recv, kv_send, raised_recv, kf_recv, o_send, o_recv, f_send, f_recv, part_send, part_recv,
):
    z = lax.axis_index("seq")
    n_z = lax.axis_size("seq")
    me = lax.axis_index("uly")
    y, x = me // 4, lax.rem(me, 4)
    below, above = z > 0, z < n_z - 1
    to_lower = {"seq": jnp.maximum(z - 1, 0)}
    to_upper = {"seq": jnp.minimum(z + 1, n_z - 1)}

    def peer(place):
        dy, dx = PLACES[place]
        return lax.rem(y + dy, 2) * 4 + lax.rem(x + dx, 4)

    def has(level):
        return z < n_z - level

    def columns_of(device, h):
        return pl.ds(pl.multiple_of((device * 2 + h) * HEAD_DIM, HEAD_DIM), HEAD_DIM)

    def place_rows(p):
        return pl.ds(p * 128, 128)

    barrier = pltpu.get_barrier_semaphore()
    for p in range(1, 8):
        pl.semaphore_signal(barrier, inc=1, device_id={"uly": peer(p)}, device_id_type=MESH)

    @pl.when(below)
    def _():
        pl.semaphore_signal(barrier, inc=1, device_id=to_lower, device_id_type=MESH)

    @pl.when(above)
    def _():
        for p in range(8):
            upper = {"seq": jnp.minimum(z + 1, n_z - 1), "uly": peer(p)}
            pl.semaphore_signal(barrier, inc=1, device_id=upper, device_id_type=MESH)

    gathered = ((q_hbm, qs, qb), (k_hbm, ks, kb), (v_hbm, vs, vb))

    def exchange_sem(t, h):
        return (q_ex if t == 0 else kv_ex).at[h]

    def own_copy(t, h):
        src, _staged, dst = gathered[t]
        return pltpu.make_async_copy(src.at[:, columns_of(me, h)], dst.at[h, place_rows(0)], exchange_sem(t, h))

    def exchange(t, h, p):
        _src, staged, dst = gathered[t]
        to = peer(MIRROR[p])
        return pltpu.make_async_remote_copy(
            src_ref=staged.at[:, columns_of(to, h)], dst_ref=dst.at[h, place_rows(p)],
            send_sem=ex_send.at[0], recv_sem=exchange_sem(t, h), device_id={"uly": to}, device_id_type=MESH,
        )

    def stage(t):
        return pltpu.make_async_copy(gathered[t][0], gathered[t][1], stage_sem.at[t])

    stored = [
        pltpu.make_async_copy(src, dst, stage_sem.at[3 + i])
        for i, (src, dst) in enumerate(((past_hbm, past), (slot_hbm, slot), (table_hbm, table)))
    ]
    for t in range(3):
        stage(t).start()
    for h in range(2):
        for t in range(3):
            own_copy(t, h).start()
    for copy in stored:
        copy.start()

    def no_parts():
        o_in[...] = jnp.zeros_like(o_in)
        l_in[...] = jnp.full_like(l_in, -1e30)
        part_in[1] = jnp.zeros(part_in.shape[1:], BF16)
        part_log_in[1] = jnp.full(part_log_in.shape[1:], -1e30, F32)
        kf[...] = jnp.zeros_like(kf)
        vf[...] = jnp.zeros_like(vf)

    def stored_sum():
        for copy in stored:
            copy.wait()
        coefs = [table[0, slot[i]] + table[1, slot[i]] for i in range(2)]

        def rows_sum(i, carry):
            rows = pl.ds(pl.multiple_of(i * 16, 16), 16)
            base[rows] = past[0, rows].astype(F32) * coefs[0] + past[1, rows].astype(F32) * coefs[1]
            return carry

        lax.fori_loop(0, 8, rows_sum, 0)

    pl.semaphore_wait(barrier, 7 + jnp.where(below, 8, 0) + jnp.where(above, 1, 0))

    blocks = (qb, q1, q2, q3)

    def split(chunk):
        return chunk // 8, place_rows(chunk % 8)

    def chunk_base(level):
        return 8 if level == 2 and MODES[0][1] < 3 else 0

    def query_sem(level, chunk):
        if level == 0:
            return o_recv.at[chunk]
        return q_recv.at[(level - 1) * 16 + chunk - chunk_base(level - 1)]

    def lower_piece(chunk):
        h, rows = split(chunk)
        to = peer(MIRROR[chunk % 8])
        return pltpu.make_async_remote_copy(
            src_ref=qs.at[:, columns_of(to, h)], dst_ref=q1.at[h, rows], send_sem=q_send.at[0],
            recv_sem=query_sem(1, chunk), device_id={"seq": jnp.maximum(z - 1, 0), "uly": to}, device_id_type=MESH,
        )

    def down(level, chunk):
        h, rows = split(chunk)
        return pltpu.make_async_remote_copy(
            src_ref=blocks[level].at[h, rows], dst_ref=blocks[level + 1].at[h, rows],
            send_sem=q_send.at[level], recv_sem=query_sem(level + 1, chunk), device_id=to_lower, device_id_type=MESH,
        )

    def raise_piece(t, p):
        _src, staged, _dst = gathered[t]
        dst = (None, kf, vf)[t].at[place_rows(0)] if p == 0 else raised.at[t - 1, p]
        return pltpu.make_async_remote_copy(
            src_ref=staged.at[:, columns_of(peer(p), RAISED)], dst_ref=dst, send_sem=kv_send,
            recv_sem=kf_recv if p == 0 else raised_recv.at[p], device_id=to_upper, device_id_type=MESH,
        )

    def pass_on(t, p):
        dst = (None, kf, vf)[t]
        return pltpu.make_async_remote_copy(
            src_ref=raised.at[t - 1, p], dst_ref=dst.at[place_rows(MIRROR[p])], send_sem=ex_send.at[1],
            recv_sem=kf_recv, device_id={"uly": peer(p)}, device_id_type=MESH,
        )

    def up(level, chunk):
        to, recv, targets = to_upper, query_sem(level, chunk), (o_in.at[level, chunk], l_in.at[level, chunk])
        if level == 0 and chunk in DIRECT:
            at = chunk // 8 * 8 + MIRROR[chunk % 8]
            to = {"seq": to_upper["seq"], "uly": peer(chunk % 8)}
            recv, targets = part_recv.at[at], (part_in.at[1, at], part_log_in.at[1, at])
        return [
            pltpu.make_async_remote_copy(
                src_ref=src.at[level, chunk], dst_ref=dst, send_sem=o_send.at[level], recv_sem=recv, device_id=to,
                device_id_type=MESH,
            )
            for src, dst in zip((o_out, l_out), targets)
        ]

    def own_part(chunk):
        at = chunk // 8 * 8 + MIRROR[chunk % 8]
        return [
            pltpu.make_async_remote_copy(
                src_ref=src.at[chunk], dst_ref=dst.at[0, at], send_sem=part_send, recv_sem=part_recv.at[at],
                device_id={"uly": peer(chunk % 8)}, device_id_type=MESH,
            )
            for src, dst in ((part_out, part_in), (part_log_out, part_log_in))
        ]

    def arrived(semaphore, count):
        pltpu.make_async_copy(tally.at[pl.ds(0, count)], tally.at[pl.ds(0, count)], semaphore).wait()

    def finish(chunk):
        h, rows = split(chunk)
        place = chunk % 8
        return pltpu.make_async_remote_copy(
            src_ref=ready.at[h, rows], dst_ref=came.at[MIRROR[place], h], send_sem=f_send,
            recv_sem=f_recv.at[batch_of(chunk)], device_id={"uly": peer(place)}, device_id_type=MESH,
        )

    done = set()

    def expect(*wanted):
        by_condition = {}
        for condition, key, copies in wanted:
            if key not in done:
                done.add(key)
                by_condition.setdefault(id(condition), (condition, []))[1].extend(copies)
        for condition, copies in by_condition.values():

            def wait(copies=copies):
                for copy in copies:
                    copy()

            if condition is None:
                wait()
            else:
                pl.when(condition)(wait)

    exists = [None, has(1), has(2), has(3)]
    came_up = [below, has(1) & below, has(2) & below]

    def queries(level, chunk):
        if level == 0:
            h = chunk // 8
            return (None, ("own", h), [functools.partial(arrived, q_ex.at[h], 512)])
        return (exists[level], ("down", level, chunk), [functools.partial(arrived, query_sem(level, chunk), 64)])

    def part(level, chunk):
        return (came_up[level], ("up", level, chunk), [functools.partial(arrived, query_sem(level, chunk), 65)])

    def in_vmem(t):
        return (None, ("in_vmem", t), [lambda: stage(t).wait()])

    def first_stage(step, pair, buffer):
        level = int(step[1])
        h, rows = pair // 4, pl.ds((pair % 4) * 256, 256)
        source = blocks[level]
        if level == 3 and h == RAISED:
            source = q2
        query = source[h, rows]
        tops = []
        for b in range(4):
            of_keys = pl.ds(b * 256, 256)
            keys = kf[of_keys] if level == 3 and h == RAISED else kb[h, of_keys]
            s = lax.dot_general(keys, query, NT, preferred_element_type=F32)
            if level == 0:
                key_row = lax.broadcasted_iota(jnp.int32, (256, 1), 0)
                query_row = lax.broadcasted_iota(jnp.int32, (1, 256), 1)
                key_pos = jnp.where(key_row < 128, peer(2 * b) * 128, peer(2 * b + 1) * 128 - 128) + key_row
                first = 2 * (pair % 4)
                query_pos = jnp.where(query_row < 128, peer(first) * 128, peer(first + 1) * 128 - 128) + query_row
                s = jnp.where(key_pos <= query_pos, s, -1e30)
            scores[buffer, pl.ds(b * 256, 256)] = s
            tops.append(jnp.max(s.reshape(32, 8, 256), axis=0))
        tops = jnp.maximum(jnp.maximum(tops[0], tops[1]), jnp.maximum(tops[2], tops[3]))
        return jnp.max(tops, axis=0, keepdims=True)

    def second_stage(step, pair, buffer, highest):
        level = int(step[1])
        h = pair // 4
        total = jnp.zeros((8, 256), F32)
        weighted = None
        for b in range(4):
            prob = jnp.exp2((scores[buffer, pl.ds(b * 256, 256)] - highest) * SCALE)
            total += jnp.sum(prob.reshape(32, 8, 256), axis=0)
            of_keys = pl.ds(b * 256, 256)
            values = vft[:, of_keys] if level == 3 and h == RAISED else vt[h, :, of_keys]
            term = lax.dot_general(values, prob.astype(BF16), NN, preferred_element_type=F32)
            weighted = term if weighted is None else weighted + term
        return weighted, jnp.sum(total, axis=0, keepdims=True)

    pending = []
    turn = [0]

    def advance(step=None, pair=None):
        last = pending.pop() if pending else None
        if step is not None:
            buffer = turn[0] % 2
            turn[0] += 1
            level = int(step[1])
            highest = first_stage(step, pair, buffer)
        if last is not None:
            old_step, old_pair, old_buffer = last
            old = int(old_step[1])
            old_top = top[old, old_pair]
            weighted, total = second_stage(old_step, old_pair, old_buffer, old_top)
            if old == 3 and MODES[old_pair // 4][1] == 3:
                mean = (weighted / total).astype(BF16)
                log_total = old_top * SCALE + jnp.log2(total)
                for i in range(2):
                    o_out[2, 2 * old_pair + i] = mean[:, i * 128 : i * 128 + 128]
                    l_out[2, 2 * old_pair + i] = log_total[:, i * 128 : i * 128 + 128]
            else:
                acc[old, old_pair] = weighted
                tot[old, old_pair] = total
                for chunk in (2 * old_pair, 2 * old_pair + 1):
                    if old == 0 and chunk in DIRECT:
                        lanes = slice(chunk % 2 * 128, chunk % 2 * 128 + 128)
                        part_out[chunk] = (weighted / total)[:, lanes].astype(BF16)
                        part_log_out[chunk] = (old_top * SCALE + jnp.log2(total))[:, lanes]
                        for copy in own_part(chunk):
                            copy.start()
                if old == 3:
                    top[old, old_pair] = jnp.where(below, old_top, -1e30)
        if step is not None:
            top[level, pair] = highest
            pending.append((step, pair, buffer))
        if last is not None and old == 3 and MODES[old_pair // 4][1] == 3:

            @pl.when(has(3))
            def _():
                for i in range(2):
                    for copy in up(2, 2 * old_pair + i):
                        copy.start()

    def settle(*units):
        if pending and pending[0][:2] in units:
            advance()

    def merged(chunk, level):
        pair, lanes = chunk // 2, slice(chunk % 2 * 128, chunk % 2 * 128 + 128)
        own = top[level, pair][:, lanes] * SCALE
        if level == 2 and MODES[chunk // 8][0] == 1:
            new = top[3, pair][:, lanes] * SCALE
            new_total, new_weighted = tot[3, pair][:, lanes], acc[3, pair, :, lanes]
        else:
            new = l_in[level, chunk]
            new_total, new_weighted = 1.0, o_in[level, chunk].astype(F32)
        most = jnp.maximum(own, new)
        a, b = jnp.exp2(own - most), jnp.exp2(new - most)
        total = tot[level, pair][:, lanes] * a + new_total * b
        weighted = acc[level, pair, :, lanes] * a + new_weighted * b
        return weighted / total, most + jnp.log2(total)

    def run(step, which):
        if step == "S0":
            expect(in_vmem(0))
            pl.when(below)(lower_piece(which).start)
        elif step in ("R1", "R2"):
            level = int(step[1])
            expect(queries(level, which))
            pl.when(has(level) & below)(down(level, which).start)
        elif step == "FL":
            advance()
        elif step == "XI":
            for code in EXCHANGE[which * 7 : which * 7 + 7]:
                expect(in_vmem(code // 16))
                exchange(code // 16, code // 8 % 2, code % 8).start()
        elif step == "SK":
            expect(in_vmem(1), in_vmem(2))

            @pl.when(above)
            def _():
                for t in (1, 2):
                    raise_piece(t, which).start()
        elif step == "XK":
            expect((below, ("raised", which), [functools.partial(arrived, raised_recv.at[which], 128)]))

            @pl.when(below)
            def _():
                for t in (1, 2):
                    pass_on(t, which).start()
        elif step == "KV":
            expect((None, ("keys", which), [functools.partial(arrived, kv_ex.at[which], 1024)]))
            vt[which] = jnp.transpose(vb[which])
        elif step == "KF":
            expect((below, ("raised",), [functools.partial(arrived, kf_recv, 1024)]))
            vft[...] = jnp.transpose(vf[...])
        elif step[0] == "C":
            level = int(step[1])
            if level == 3 and MODES[which // 4][0] == 1:
                level = 2
            expect(queries(level, 2 * which), queries(level, 2 * which + 1))
            advance(step, which)
        elif step == "M0" and which in DIRECT:
            settle(("C0", which // 2))
            h, place = which // 8, MIRROR[which % 8]
            at = h * 8 + place
            pl.when(below)(functools.partial(arrived, part_recv.at[at], 130))
            pl.when(z == 0)(functools.partial(arrived, part_recv.at[at], 65))
            most = jnp.maximum(part_log_in[0, at], part_log_in[1, at])
            a, b = (jnp.exp2(part_log_in[i, at] - most) for i in range(2))
            mean = (part_in[0, at].astype(F32) * a + part_in[1, at].astype(F32) * b) / (a + b)
            attended = jnp.transpose(mean).astype(BF16).astype(F32)
            lanes = columns_of(peer(place), h)
            out[:, lanes] = (base[:, lanes] + attended).astype(BF16)
        elif step == "M0":
            settle(("C0", which // 2))
            expect(part(0, which))
            mean, _unused = merged(which, 0)
            h, rows = split(which)
            if which % 8 == 0:
                came[0, h] = jnp.transpose(mean).astype(BF16)
            else:
                ready[h, rows] = jnp.transpose(mean).astype(BF16)
                finish(which).start()
        else:
            level = int(step[1])
            if level == 2 and MODES[which // 8][0] == 1:
                settle(("C2", which // 2), ("C3", which // 2))
            else:
                settle((f"C{level}", which // 2))
                expect(part(level, which))
            mean, log_total = merged(which, level)
            o_out[level - 1, which] = mean.astype(BF16)
            l_out[level - 1, which] = log_total

            @pl.when(has(level))
            def _(level=level, which=which):
                for copy in up(level - 1, which):
                    copy.start()

    summed = False
    for code in ORDER:
        step, which = STEPS[code // 16], code % 16
        if not summed and step not in ("XI", "SK", "S0"):
            pl.when(z == 0)(no_parts)
            stored_sum()
            summed = True
        ns = PAUSES.get(code)
        if ns:
            pl.when(lax.rem(lax.axis_index("rep"), 2) == 1)(functools.partial(pl.delay, ns))
        ns = LATE_PAUSES.get(code)
        if ns:
            pl.when((lax.axis_index("rep") == 1) & (z < 4))(functools.partial(pl.delay, ns))
        run(step, which)

    for batch, (first, last) in enumerate(BATCHES):
        chunks = M0S[first:last]
        remote = sum(1 for chunk in chunks if chunk % 8)
        if remote:
            arrived(f_recv.at[batch], remote * 64)
        for chunk in chunks:
            h, place = chunk // 8, MIRROR[chunk % 8]
            lanes = columns_of(peer(place), h)
            out[:, lanes] = (base[:, lanes] + came[place, h].astype(F32)).astype(BF16)

    sent = scores.at[:, pl.ds(0, 672)]
    pltpu.make_async_copy(sent, sent, ex_send.at[0]).wait()
    arrived(f_send, 64 * (14 - len(DIRECT)))
    if DIRECT:
        arrived(part_send, 65 * len(DIRECT))
    pl.when(below)(functools.partial(arrived, ex_send.at[1], 896))
    pl.when(above)(functools.partial(arrived, kv_send, 1024))
    for level in range(3):
        heads = sum(1 for _up_hops, down_hops in MODES if down_hops > level)
        pl.when(has(level) & below)(functools.partial(arrived, q_send.at[level], 512 * heads))
        pl.when(has(level + 1))(functools.partial(arrived, o_send.at[level], 520 * heads))


def attention(slot, table, queries, keys, values, past):
    block = pltpu.VMEM((2, 1024, HEAD_DIM), BF16)
    turned = pltpu.VMEM((2, HEAD_DIM, 1024), BF16)
    staged = pltpu.VMEM(queries.shape, BF16)
    parts, logs = (3, 16, HEAD_DIM, 128), (3, 16, 1, 128)
    dma = pltpu.SemaphoreType.DMA
    chunks = 32 + 8 * sum(1 for _up_hops, down_hops in MODES if down_hops == 3)
    return pl.pallas_call(
        kernel,
        out_shape=pltpu.VMEM(queries.shape, BF16),
        in_specs=[pl.BlockSpec(memory_space=pl.ANY)] * 6,
        scratch_shapes=[
            pltpu.SMEM(slot.shape, jnp.int32), pltpu.SMEM(table.shape, F32), staged, staged, staged,
            pltpu.VMEM(past.shape, BF16), pltpu.VMEM(queries.shape, F32), pltpu.VMEM((1040, 1, 128), F32),
            block, block, block, turned, block, block, block, pltpu.VMEM((2, 8, 128, HEAD_DIM), BF16),
            pltpu.VMEM((1024, HEAD_DIM), BF16), pltpu.VMEM((1024, HEAD_DIM), BF16), pltpu.VMEM((HEAD_DIM, 1024), BF16),
            pltpu.VMEM(parts, BF16), pltpu.VMEM(logs, F32), pltpu.VMEM(parts, BF16), pltpu.VMEM(logs, F32),
            pltpu.VMEM((4, 8, HEAD_DIM, 256), F32), pltpu.VMEM((4, 8, 1, 256), F32), pltpu.VMEM((4, 8, 1, 256), F32),
            pltpu.VMEM((2, 1024, 256), F32), block, pltpu.VMEM((8, 2, 128, HEAD_DIM), BF16),
            pltpu.VMEM(parts[1:], BF16), pltpu.VMEM(logs[1:], F32),
            pltpu.VMEM((2, *parts[1:]), BF16), pltpu.VMEM((2, *logs[1:]), F32),
            dma((6,)), dma((2,)), dma((2,)), dma((2,)), dma((3,)), dma((chunks,)), dma(()), dma((8,)), dma(()),
            dma((3,)), dma((16,)), dma(()), dma((len(BATCHES),)), dma(()), dma((16,)),
        ],
        compiler_params=pltpu.CompilerParams(collective_id=0, has_side_effects=True),
        name="attention",
    )(slot, table, queries, keys, values, past)


def shards(queries, keys, values, past_outputs, dwa_slot, dwa_table):
    return attention(dwa_slot, dwa_table, queries, keys, values, past_outputs)


def solution(mesh):
    tokens = P(("rep", "seq", "uly"), None)
    return jax.shard_map(
        shards,
        mesh=mesh,
        in_specs=(tokens, tokens, tokens, P(None, ("rep", "seq", "uly"), None), P(), P()),
        out_specs=tokens,
        check_vma=False,
    )
```

```python
import functools
import math

import jax
import jax.numpy as jnp
from jax import lax
from jax.experimental import pallas as pl
from jax.experimental.pallas import tpu as pltpu
from jax.sharding import PartitionSpec as P

MESH = pl.DeviceIdType.MESH
HEAD_DIM = 128
SCALE = math.log2(math.e) / math.sqrt(HEAD_DIM)
BF16, F32 = jnp.bfloat16, jnp.float32
NT = (((1,), (1,)), ((), ()))
NN = (((1,), (0,)), ((), ()))

PLACES = ((0, 0), (0, 1), (0, 3), (1, 0), (1, 1), (1, 3), (0, 2), (1, 2))
MIRROR = tuple(PLACES.index((dy, (4 - dx) % 4)) for dy, dx in PLACES)

MODES = ((1, 2), (0, 3))
RAISED = next(h for h, (up_hops, _down_hops) in enumerate(MODES) if up_hops)
EXCHANGE = (
    25, 26, 27, 28, 29, 30, 31, 41, 42, 43, 44, 45, 46, 47, 17, 18, 19, 20, 21, 22, 23, 33, 34, 35,
    36, 37, 38, 39, 9, 10, 11, 12, 13, 14, 15, 1, 2, 3, 4, 5, 6, 7,
)

STEPS = ("S0", "R1", "R2", "C3", "C2", "C1", "C0", "M2", "M1", "M0", "KV", "KF", "SK", "XK", "XI", "FL")
DIRECT = (1, 2, 3, 9)
ORDER = (
    12, 192, 13, 197, 199, 196, 15, 195, 193, 11, 194, 10, 14, 198, 9, 224, 225, 226, 28, 29, 27, 26, 31, 215,
    30, 212, 44, 45, 43, 42, 210, 47, 46, 6, 7, 8, 4, 25, 161, 0, 5, 209, 69, 70, 227, 54, 240, 53,
    240, 55, 240, 124, 1, 213, 86, 2, 240, 122, 214, 24, 3, 125, 22, 71, 87, 84, 23, 85, 211, 123, 228, 126,
    20, 240, 140, 21, 127, 141, 160, 40, 138, 68, 41, 80, 16, 17, 142, 83, 82, 139, 67, 176, 18, 143, 51, 119,
    229, 118, 19, 66, 50, 116, 81, 117, 52, 101, 103, 154, 135, 159, 134, 102, 155, 158, 48, 65, 156, 133, 157, 132,
    49, 64, 113, 121, 114, 99, 98, 151, 150, 120, 115, 100, 149, 96, 240, 129, 112, 137, 148, 130, 131, 97, 136, 240,
    145, 128, 146, 153, 147, 152, 144,
)


PAUSES = {STEPS.index("M2") * 16 + 12: 2000}
LATE_PAUSES = {STEPS.index("M2") * 16 + 12: 2000}

PARTS_AT = tuple(chunk // 8 * 8 + MIRROR[chunk % 8] for chunk in DIRECT)

M0S = tuple(code % 16 for code in ORDER if STEPS[code // 16] == "M0" and code % 16 not in DIRECT)
BATCHES = ((0, 8), (8, len(M0S) - 2), (len(M0S) - 2, len(M0S) - 1), (len(M0S) - 1, len(M0S)))


def batch_of(chunk):
    at = M0S.index(chunk)
    return next(i for i, (first, last) in enumerate(BATCHES) if first <= at < last)


def kernel(
    slot_hbm, table_hbm, q_hbm, k_hbm, v_hbm, past_hbm, out,
    slot, table, qs, ks, vs, past, base, tally,
    qb, kb, vb, vt, q1, q2, q3, raised, kf, vf, vft, o_in, l_in, o_out, l_out, acc, top, tot, scores, ready, came,
    part_out, part_log_out, part_in, part_log_in,
    stage_sem, ex_send, q_ex, kv_ex, q_send, q_recv, kv_send, raised_recv, kf_recv, o_send, o_recv, f_send, f_recv, part_send, part_recv,
):
    z = lax.axis_index("seq")
    n_z = lax.axis_size("seq")
    me = lax.axis_index("uly")
    y, x = me // 4, lax.rem(me, 4)
    below, above = z > 0, z < n_z - 1
    to_lower = {"seq": jnp.maximum(z - 1, 0)}
    to_upper = {"seq": jnp.minimum(z + 1, n_z - 1)}

    def peer(place):
        dy, dx = PLACES[place]
        return lax.rem(y + dy, 2) * 4 + lax.rem(x + dx, 4)

    def has(level):
        return z < n_z - level

    def columns_of(device, h):
        return pl.ds(pl.multiple_of((device * 2 + h) * HEAD_DIM, HEAD_DIM), HEAD_DIM)

    def place_rows(p):
        return pl.ds(p * 128, 128)

    barrier = pltpu.get_barrier_semaphore()
    for p in range(1, 8):
        pl.semaphore_signal(barrier, inc=1, device_id={"uly": peer(p)}, device_id_type=MESH)

    @pl.when(below)
    def _():
        pl.semaphore_signal(barrier, inc=1, device_id=to_lower, device_id_type=MESH)

    @pl.when(above)
    def _():
        for p in range(8):
            upper = {"seq": jnp.minimum(z + 1, n_z - 1), "uly": peer(p)}
            pl.semaphore_signal(barrier, inc=1, device_id=upper, device_id_type=MESH)

    gathered = ((q_hbm, qs, qb), (k_hbm, ks, kb), (v_hbm, vs, vb))

    def exchange_sem(t, h):
        return (q_ex if t == 0 else kv_ex).at[h]

    def own_copy(t, h):
        src, _staged, dst = gathered[t]
        return pltpu.make_async_copy(src.at[:, columns_of(me, h)], dst.at[h, place_rows(0)], exchange_sem(t, h))

    def exchange(t, h, p):
        _src, staged, dst = gathered[t]
        to = peer(MIRROR[p])
        return pltpu.make_async_remote_copy(
            src_ref=staged.at[:, columns_of(to, h)], dst_ref=dst.at[h, place_rows(p)],
            send_sem=ex_send.at[0], recv_sem=exchange_sem(t, h), device_id={"uly": to}, device_id_type=MESH,
        )

    def stage(t):
        return pltpu.make_async_copy(gathered[t][0], gathered[t][1], stage_sem.at[t])

    stored = [
        pltpu.make_async_copy(src, dst, stage_sem.at[3 + i])
        for i, (src, dst) in enumerate(((past_hbm, past), (slot_hbm, slot), (table_hbm, table)))
    ]
    for t in range(3):
        stage(t).start()
    for h in range(2):
        for t in range(3):
            own_copy(t, h).start()
    for copy in stored:
        copy.start()

    def no_parts():
        o_in[...] = jnp.zeros_like(o_in)
        l_in[...] = jnp.full_like(l_in, -1e30)
        part_in[1] = jnp.zeros(part_in.shape[1:], BF16)
        part_log_in[1] = jnp.full(part_log_in.shape[1:], -1e30, F32)
        kf[...] = jnp.zeros_like(kf)
        vf[...] = jnp.zeros_like(vf)

    def stored_sum():
        for copy in stored:
            copy.wait()
        coefs = [table[0, slot[i]] + table[1, slot[i]] for i in range(2)]

        def rows_sum(i, carry):
            rows = pl.ds(pl.multiple_of(i * 16, 16), 16)
            base[rows] = past[0, rows].astype(F32) * coefs[0] + past[1, rows].astype(F32) * coefs[1]
            return carry

        lax.fori_loop(0, 8, rows_sum, 0)

    pl.semaphore_wait(barrier, 7 + jnp.where(below, 8, 0) + jnp.where(above, 1, 0))

    blocks = (qb, q1, q2, q3)

    def split(chunk):
        return chunk // 8, place_rows(chunk % 8)

    def chunk_base(level):
        return 8 if level == 2 and MODES[0][1] < 3 else 0

    def query_sem(level, chunk):
        if level == 0:
            return o_recv.at[chunk]
        return q_recv.at[(level - 1) * 16 + chunk - chunk_base(level - 1)]

    def lower_piece(chunk):
        h, rows = split(chunk)
        to = peer(MIRROR[chunk % 8])
        return pltpu.make_async_remote_copy(
            src_ref=qs.at[:, columns_of(to, h)], dst_ref=q1.at[h, rows], send_sem=q_send.at[0],
            recv_sem=query_sem(1, chunk), device_id={"seq": jnp.maximum(z - 1, 0), "uly": to}, device_id_type=MESH,
        )

    def down(level, chunk):
        h, rows = split(chunk)
        return pltpu.make_async_remote_copy(
            src_ref=blocks[level].at[h, rows], dst_ref=blocks[level + 1].at[h, rows],
            send_sem=q_send.at[level], recv_sem=query_sem(level + 1, chunk), device_id=to_lower, device_id_type=MESH,
        )

    def raise_piece(t, p):
        _src, staged, _dst = gathered[t]
        dst = (None, kf, vf)[t].at[place_rows(0)] if p == 0 else raised.at[t - 1, p]
        return pltpu.make_async_remote_copy(
            src_ref=staged.at[:, columns_of(peer(p), RAISED)], dst_ref=dst, send_sem=kv_send,
            recv_sem=kf_recv if p == 0 else raised_recv.at[p], device_id=to_upper, device_id_type=MESH,
        )

    def pass_on(t, p):
        dst = (None, kf, vf)[t]
        return pltpu.make_async_remote_copy(
            src_ref=raised.at[t - 1, p], dst_ref=dst.at[place_rows(MIRROR[p])], send_sem=ex_send.at[1],
            recv_sem=kf_recv, device_id={"uly": peer(p)}, device_id_type=MESH,
        )

    def up(level, chunk):
        to, recv, targets = to_upper, query_sem(level, chunk), (o_in.at[level, chunk], l_in.at[level, chunk])
        if level == 0 and chunk in DIRECT:
            at = chunk // 8 * 8 + MIRROR[chunk % 8]
            to = {"seq": to_upper["seq"], "uly": peer(chunk % 8)}
            recv, targets = part_recv.at[PARTS_AT.index(at)], (part_in.at[1, at], part_log_in.at[1, at])
        return [
            pltpu.make_async_remote_copy(
                src_ref=src.at[level, chunk], dst_ref=dst, send_sem=o_send.at[level], recv_sem=recv, device_id=to,
                device_id_type=MESH,
            )
            for src, dst in zip((o_out, l_out), targets)
        ]

    def own_part(chunk):
        at = chunk // 8 * 8 + MIRROR[chunk % 8]
        return [
            pltpu.make_async_remote_copy(
                src_ref=src.at[chunk], dst_ref=dst.at[0, at], send_sem=part_send, recv_sem=part_recv.at[PARTS_AT.index(at)],
                device_id={"uly": peer(chunk % 8)}, device_id_type=MESH,
            )
            for src, dst in ((part_out, part_in), (part_log_out, part_log_in))
        ]

    def arrived(semaphore, count):
        pltpu.make_async_copy(tally.at[pl.ds(0, count)], tally.at[pl.ds(0, count)], semaphore).wait()

    def finish(chunk):
        h, rows = split(chunk)
        place = chunk % 8
        return pltpu.make_async_remote_copy(
            src_ref=ready.at[h, rows], dst_ref=came.at[MIRROR[place], h], send_sem=f_send,
            recv_sem=f_recv.at[batch_of(chunk)], device_id={"uly": peer(place)}, device_id_type=MESH,
        )

    done = set()

    def expect(*wanted):
        by_condition = {}
        for condition, key, copies in wanted:
            if key not in done:
                done.add(key)
                by_condition.setdefault(id(condition), (condition, []))[1].extend(copies)
        for condition, copies in by_condition.values():

            def wait(copies=copies):
                for copy in copies:
                    copy()

            if condition is None:
                wait()
            else:
                pl.when(condition)(wait)

    exists = [None, has(1), has(2), has(3)]
    came_up = [below, has(1) & below, has(2) & below]

    def queries(level, chunk):
        if level == 0:
            h = chunk // 8
            return (None, ("own", h), [functools.partial(arrived, q_ex.at[h], 512)])
        return (exists[level], ("down", level, chunk), [functools.partial(arrived, query_sem(level, chunk), 64)])

    def part(level, chunk):
        return (came_up[level], ("up", level, chunk), [functools.partial(arrived, query_sem(level, chunk), 65)])

    def in_vmem(t):
        return (None, ("in_vmem", t), [lambda: stage(t).wait()])

    def first_stage(step, pair, buffer):
        level = int(step[1])
        h, rows = pair // 4, pl.ds((pair % 4) * 256, 256)
        source = blocks[level]
        if level == 3 and h == RAISED:
            source = q2
        query = source[h, rows]
        tops = []
        for b in range(4):
            of_keys = pl.ds(b * 256, 256)
            keys = kf[of_keys] if level == 3 and h == RAISED else kb[h, of_keys]
            s = lax.dot_general(keys, query, NT, preferred_element_type=F32)
            if level == 0:
                key_row = lax.broadcasted_iota(jnp.int32, (256, 1), 0)
                query_row = lax.broadcasted_iota(jnp.int32, (1, 256), 1)
                key_pos = jnp.where(key_row < 128, peer(2 * b) * 128, peer(2 * b + 1) * 128 - 128) + key_row
                first = 2 * (pair % 4)
                query_pos = jnp.where(query_row < 128, peer(first) * 128, peer(first + 1) * 128 - 128) + query_row
                s = jnp.where(key_pos <= query_pos, s, -1e30)
            scores[buffer, pl.ds(b * 256, 256)] = s
            tops.append(jnp.max(s.reshape(32, 8, 256), axis=0))
        tops = jnp.maximum(jnp.maximum(tops[0], tops[1]), jnp.maximum(tops[2], tops[3]))
        return jnp.max(tops, axis=0, keepdims=True)

    def second_stage(step, pair, buffer, highest):
        level = int(step[1])
        h = pair // 4
        total = jnp.zeros((8, 256), F32)
        weighted = None
        for b in range(4):
            prob = jnp.exp2((scores[buffer, pl.ds(b * 256, 256)] - highest) * SCALE)
            total += jnp.sum(prob.reshape(32, 8, 256), axis=0)
            of_keys = pl.ds(b * 256, 256)
            values = vft[:, of_keys] if level == 3 and h == RAISED else vt[h, :, of_keys]
            term = lax.dot_general(values, prob.astype(BF16), NN, preferred_element_type=F32)
            weighted = term if weighted is None else weighted + term
        return weighted, jnp.sum(total, axis=0, keepdims=True)

    pending = []
    turn = [0]

    def advance(step=None, pair=None):
        last = pending.pop() if pending else None
        if step is not None:
            buffer = turn[0] % 2
            turn[0] += 1
            level = int(step[1])
            highest = first_stage(step, pair, buffer)
        if last is not None:
            old_step, old_pair, old_buffer = last
            old = int(old_step[1])
            old_top = top[old, old_pair]
            weighted, total = second_stage(old_step, old_pair, old_buffer, old_top)
            if old == 3 and MODES[old_pair // 4][1] == 3:
                mean = (weighted / total).astype(BF16)
                log_total = old_top * SCALE + jnp.log2(total)
                for i in range(2):
                    o_out[2, 2 * old_pair + i] = mean[:, i * 128 : i * 128 + 128]
                    l_out[2, 2 * old_pair + i] = log_total[:, i * 128 : i * 128 + 128]
            else:
                acc[old, old_pair] = weighted
                tot[old, old_pair] = total
                for chunk in (2 * old_pair, 2 * old_pair + 1):
                    if old == 0 and chunk in DIRECT:
                        lanes = slice(chunk % 2 * 128, chunk % 2 * 128 + 128)
                        part_out[chunk] = (weighted / total)[:, lanes].astype(BF16)
                        part_log_out[chunk] = (old_top * SCALE + jnp.log2(total))[:, lanes]
                        for copy in own_part(chunk):
                            copy.start()
                if old == 3:
                    top[old, old_pair] = jnp.where(below, old_top, -1e30)
        if step is not None:
            top[level, pair] = highest
            pending.append((step, pair, buffer))
        if last is not None and old == 3 and MODES[old_pair // 4][1] == 3:

            @pl.when(has(3))
            def _():
                for i in range(2):
                    for copy in up(2, 2 * old_pair + i):
                        copy.start()

    def settle(*units):
        if pending and pending[0][:2] in units:
            advance()

    def merged(chunk, level):
        pair, lanes = chunk // 2, slice(chunk % 2 * 128, chunk % 2 * 128 + 128)
        own = top[level, pair][:, lanes] * SCALE
        if level == 2 and MODES[chunk // 8][0] == 1:
            new = top[3, pair][:, lanes] * SCALE
            new_total, new_weighted = tot[3, pair][:, lanes], acc[3, pair, :, lanes]
        else:
            new = l_in[level, chunk]
            new_total, new_weighted = 1.0, o_in[level, chunk].astype(F32)
        most = jnp.maximum(own, new)
        a, b = jnp.exp2(own - most), jnp.exp2(new - most)
        total = tot[level, pair][:, lanes] * a + new_total * b
        weighted = acc[level, pair, :, lanes] * a + new_weighted * b
        return weighted / total, most + jnp.log2(total)

    def run(step, which):
        if step == "S0":
            expect(in_vmem(0))
            pl.when(below)(lower_piece(which).start)
        elif step in ("R1", "R2"):
            level = int(step[1])
            expect(queries(level, which))
            pl.when(has(level) & below)(down(level, which).start)
        elif step == "FL":
            advance()
        elif step == "XI":
            for code in EXCHANGE[which * 7 : which * 7 + 7]:
                expect(in_vmem(code // 16))
                exchange(code // 16, code // 8 % 2, code % 8).start()
        elif step == "SK":
            expect(in_vmem(1), in_vmem(2))

            @pl.when(above)
            def _():
                for t in (1, 2):
                    raise_piece(t, which).start()
        elif step == "XK":
            expect((below, ("raised", which), [functools.partial(arrived, raised_recv.at[which], 128)]))

            @pl.when(below)
            def _():
                for t in (1, 2):
                    pass_on(t, which).start()
        elif step == "KV":
            expect((None, ("keys", which), [functools.partial(arrived, kv_ex.at[which], 1024)]))
            vt[which] = jnp.transpose(vb[which])
        elif step == "KF":
            expect((below, ("raised",), [functools.partial(arrived, kf_recv, 1024)]))
            vft[...] = jnp.transpose(vf[...])
        elif step[0] == "C":
            level = int(step[1])
            if level == 3 and MODES[which // 4][0] == 1:
                level = 2
            expect(queries(level, 2 * which), queries(level, 2 * which + 1))
            advance(step, which)
        elif step == "M0" and which in DIRECT:
            settle(("C0", which // 2))
            h, place = which // 8, MIRROR[which % 8]
            at = h * 8 + place
            pl.when(below)(functools.partial(arrived, part_recv.at[PARTS_AT.index(at)], 130))
            pl.when(z == 0)(functools.partial(arrived, part_recv.at[PARTS_AT.index(at)], 65))
            most = jnp.maximum(part_log_in[0, at], part_log_in[1, at])
            a, b = (jnp.exp2(part_log_in[i, at] - most) for i in range(2))
            mean = (part_in[0, at].astype(F32) * a + part_in[1, at].astype(F32) * b) / (a + b)
            attended = jnp.transpose(mean).astype(BF16).astype(F32)
            lanes = columns_of(peer(place), h)
            out[:, lanes] = (base[:, lanes] + attended).astype(BF16)
        elif step == "M0":
            settle(("C0", which // 2))
            expect(part(0, which))
            mean, _unused = merged(which, 0)
            h, rows = split(which)
            if which % 8 == 0:
                came[0, h] = jnp.transpose(mean).astype(BF16)
            else:
                ready[h, rows] = jnp.transpose(mean).astype(BF16)
                finish(which).start()
        else:
            level = int(step[1])
            if level == 2 and MODES[which // 8][0] == 1:
                settle(("C2", which // 2), ("C3", which // 2))
            else:
                settle((f"C{level}", which // 2))
                expect(part(level, which))
            mean, log_total = merged(which, level)
            o_out[level - 1, which] = mean.astype(BF16)
            l_out[level - 1, which] = log_total

            @pl.when(has(level))
            def _(level=level, which=which):
                for copy in up(level - 1, which):
                    copy.start()

    summed = False
    for code in ORDER:
        step, which = STEPS[code // 16], code % 16
        if not summed and step not in ("XI", "SK", "S0"):
            pl.when(z == 0)(no_parts)
            stored_sum()
            summed = True
        ns = PAUSES.get(code)
        if ns:
            pl.when(lax.rem(lax.axis_index("rep"), 2) == 1)(functools.partial(pl.delay, ns))
        ns = LATE_PAUSES.get(code)
        if ns:
            pl.when((lax.axis_index("rep") == 1) & (z < 8))(functools.partial(pl.delay, ns))
        run(step, which)

    for batch, (first, last) in enumerate(BATCHES):
        chunks = M0S[first:last]
        remote = sum(1 for chunk in chunks if chunk % 8)
        if remote:
            arrived(f_recv.at[batch], remote * 64)
        for chunk in chunks:
            h, place = chunk // 8, MIRROR[chunk % 8]
            lanes = columns_of(peer(place), h)
            out[:, lanes] = (base[:, lanes] + came[place, h].astype(F32)).astype(BF16)

    sent = scores.at[:, pl.ds(0, 672)]
    pltpu.make_async_copy(sent, sent, ex_send.at[0]).wait()
    arrived(f_send, 64 * (14 - len(DIRECT)))
    if DIRECT:
        arrived(part_send, 65 * len(DIRECT))
    pl.when(below)(functools.partial(arrived, ex_send.at[1], 896))
    pl.when(above)(functools.partial(arrived, kv_send, 1024))
    for level in range(3):
        heads = sum(1 for _up_hops, down_hops in MODES if down_hops > level)
        pl.when(has(level) & below)(functools.partial(arrived, q_send.at[level], 512 * heads))
        pl.when(has(level + 1))(functools.partial(arrived, o_send.at[level], 520 * heads))


def attention(slot, table, queries, keys, values, past):
    block = pltpu.VMEM((2, 1024, HEAD_DIM), BF16)
    turned = pltpu.VMEM((2, HEAD_DIM, 1024), BF16)
    staged = pltpu.VMEM(queries.shape, BF16)
    parts, logs = (3, 16, HEAD_DIM, 128), (3, 16, 1, 128)
    dma = pltpu.SemaphoreType.DMA
    chunks = 32 + 8 * sum(1 for _up_hops, down_hops in MODES if down_hops == 3)
    return pl.pallas_call(
        kernel,
        out_shape=pltpu.VMEM(queries.shape, BF16),
        in_specs=[pl.BlockSpec(memory_space=pl.ANY)] * 6,
        scratch_shapes=[
            pltpu.SMEM(slot.shape, jnp.int32), pltpu.SMEM(table.shape, F32), staged, staged, staged,
            pltpu.VMEM(past.shape, BF16), pltpu.VMEM(queries.shape, F32), pltpu.VMEM((1040, 1, 128), F32),
            block, block, block, turned, block, block, block, pltpu.VMEM((2, 8, 128, HEAD_DIM), BF16),
            pltpu.VMEM((1024, HEAD_DIM), BF16), pltpu.VMEM((1024, HEAD_DIM), BF16), pltpu.VMEM((HEAD_DIM, 1024), BF16),
            pltpu.VMEM(parts, BF16), pltpu.VMEM(logs, F32), pltpu.VMEM(parts, BF16), pltpu.VMEM(logs, F32),
            pltpu.VMEM((4, 8, HEAD_DIM, 256), F32), pltpu.VMEM((4, 8, 1, 256), F32), pltpu.VMEM((4, 8, 1, 256), F32),
            pltpu.VMEM((2, 1024, 256), F32), block, pltpu.VMEM((8, 2, 128, HEAD_DIM), BF16),
            pltpu.VMEM(parts[1:], BF16), pltpu.VMEM(logs[1:], F32),
            pltpu.VMEM((2, *parts[1:]), BF16), pltpu.VMEM((2, *logs[1:]), F32),
            dma((6,)), dma((2,)), dma((2,)), dma((2,)), dma((3,)), dma((chunks,)), dma(()), dma((8,)), dma(()),
            dma((3,)), dma((16,)), dma(()), dma((len(BATCHES),)), dma(()), dma((len(DIRECT),)),
        ],
        compiler_params=pltpu.CompilerParams(collective_id=0, has_side_effects=True),
        name="attention",
    )(slot, table, queries, keys, values, past)


def shards(queries, keys, values, past_outputs, dwa_slot, dwa_table):
    return attention(dwa_slot, dwa_table, queries, keys, values, past_outputs)


def solution(mesh):
    tokens = P(("rep", "seq", "uly"), None)
    return jax.shard_map(
        shards,
        mesh=mesh,
        in_specs=(tokens, tokens, tokens, P(None, ("rep", "seq", "uly"), None), P(), P()),
        out_specs=tokens,
        check_vma=False,
    )
```
